32 devices in a mesh: gz: 8 (over z, x), rows: 4 (over y, core).
Axes of the slice: x: 2, y: 2, z: 4, core: 2. Of those that a mesh axis runs over, the one named last changes fastest.
Arguments:
- sections: bfloat16 [8, 1024, 4096], P('gz', 'rows'), may hold values from -4 to 4
- peaks: int32 [8, 2, 1, 4], P('gz'), may hold values from -16 to 16, as said below
Outputs:
- field: float32 [8, 2, 1024, 4096], P('gz', None, 'rows')
- pair_offsets: float32 [8, 2, 1, 4], P('gz')
- residual: bfloat16 [8, 1024, 4096], P('gz', 'rows')
The draws below stay inside these ranges and needn't reach their ends.
Inputs may be any that keep to these rules, and one draw needn't show every extreme that they name: `peaks`: in every draw the first section's first patch has row offset 16 and column offset -16.
All inputs are finite; a program needn't handle non-finite values.
Results may differ from the reference program's by a relative error of at most 0.001.
Values may be sent and summed in bfloat16 or wider, within the bound.
A program may use at most 64 MiB of HBM per device.

```python
import jax
import jax.numpy as jnp
import numpy as np
from jax import lax

W = 4096
PATCH = 1024
MAXOFF = 16
H = 1024
SECTIONS = 8
PGY = 1
PGX = 4


def joint_shifts(key):
    peaks = jax.random.randint(jax.random.fold_in(key, 11), (SECTIONS, 2, PGY, PGX), -MAXOFF, MAXOFF + 1)
    peaks = peaks.at[0, 0, 0, 0].set(MAXOFF).at[0, 1, 0, 0].set(-MAXOFF)
    fraction = jax.random.uniform(jax.random.fold_in(key, 12), (SECTIONS, 2, PGY, PGX), minval=-0.5, maxval=0.5)
    total = jnp.cumsum(peaks.astype(jnp.float32) + fraction, axis=0)
    return (peaks, total)


def draw_peaks(key, part):
    return joint_shifts(key)[0]


def draw_sections(key, part):
    _, total = joint_shifts(key)
    waves = 12
    wave_key = jax.random.fold_in(key, 13)
    length = jnp.exp(jax.random.uniform(jax.random.fold_in(wave_key, 1), (waves,), minval=jnp.log(12.0), maxval=jnp.log(64.0)))
    heading = jax.random.uniform(jax.random.fold_in(wave_key, 2), (waves,), minval=-3.14159, maxval=3.14159)
    phase = jax.random.uniform(jax.random.fold_in(wave_key, 3), (waves,), minval=-3.14159, maxval=3.14159)
    amplitude = 0.25 * jnp.ones((waves,), jnp.float32)
    noise_scale = 0.05
    freq_y = 6.2831853 / length * jnp.sin(heading)
    freq_x = 6.2831853 / length * jnp.cos(heading)
    row_index = jnp.arange(H)
    col_index = jnp.arange(W)
    patch_y = row_index // PATCH
    patch_x = col_index // PATCH
    noise_key = jax.random.fold_in(key, 14)

    def single(index):
        shift_y = total[index, 0][patch_y][:, patch_x]
        shift_x = total[index, 1][patch_y][:, patch_x]
        coord_y = row_index.astype(jnp.float32)[:, None] + shift_y
        coord_x = col_index.astype(jnp.float32)[None, :] + shift_x
        image = jnp.zeros((H, W), jnp.float32)
        for wave in range(waves):
            image = image + amplitude[wave] * jnp.cos(freq_y[wave] * coord_y + freq_x[wave] * coord_x + phase[wave])
        noise = jax.random.normal(jax.random.fold_in(noise_key, index), (H, W)) * noise_scale
        return jnp.clip(image + noise, -4.0, 4.0)
    return lax.map(single, jnp.arange(SECTIONS)).astype(jnp.bfloat16)


def setup_inputs(seed: int = 0) -> dict:
    streams_of = jax.random.split(jax.random.key(seed), 3)
    sections = draw_sections(jax.random.fold_in(streams_of[2], 71), 0)
    peaks = draw_peaks(jax.random.fold_in(streams_of[2], 71), 0)
    return dict(sections=sections, peaks=peaks)


LAMBDA = 0.002
RIDGE = 0.05


def invert_three(matrix):
    a, b, c = matrix[0, 0], matrix[0, 1], matrix[0, 2]
    d, e, f = matrix[1, 0], matrix[1, 1], matrix[1, 2]
    g, h, k = matrix[2, 0], matrix[2, 1], matrix[2, 2]
    cof = np.array([[e * k - f * h, c * h - b * k, b * f - c * e],
                    [f * g - d * k, a * k - c * g, c * d - a * f],
                    [d * h - e * g, b * g - a * h, a * e - b * d]])
    return cof / (a * (e * k - f * h) - b * (d * k - f * g) + c * (d * h - e * g))


def fit_table(pgy, pgx, patch, height, width):
    yy = ((np.arange(pgy) + 0.5) * patch - height / 2.0) / height
    xx = ((np.arange(pgx) + 0.5) * patch - width / 2.0) / width
    design = np.stack([np.repeat(yy, pgx), np.tile(xx, pgy), np.ones(pgy * pgx)], 1)
    ridge_matrix = np.array([[RIDGE, 0.0, 0.0], [0.0, RIDGE, 0.0], [0.0, 0.0, 0.0]])
    gram = design.T @ design + ridge_matrix
    return invert_three(gram) @ design.T


def spread(count, patch, nodes, start):
    pos = (start + jnp.arange(count).astype(jnp.float32) + 0.5) / patch - 0.5
    pos = jnp.clip(pos, 0.0, nodes - 1.0)
    return jnp.maximum(0.0, 1.0 - jnp.abs(pos[:, None] - jnp.arange(nodes).astype(jnp.float32)[None, :]))


def moments(current, window):
    centre = window[1:-1, 1:-1]
    grad_y = (window[2:, 1:-1] - window[:-2, 1:-1]) * 0.5
    grad_x = (window[1:-1, 2:] - window[1:-1, :-2]) * 0.5
    error = current - centre
    sums = jnp.stack([jnp.sum(grad_y * grad_y), jnp.sum(grad_y * grad_x), jnp.sum(grad_x * grad_x),
                      jnp.sum(grad_y * error), jnp.sum(grad_x * error)])
    return sums, error


def solve_pairs(sums, peak_grid):
    damping = LAMBDA * PATCH * PATCH
    first = sums[0] + damping
    cross = sums[1]
    second = sums[2] + damping
    determinant = first * second - cross * cross
    step_y = (second * sums[3] - cross * sums[4]) / determinant
    step_x = (first * sums[4] - cross * sums[3]) / determinant
    return peak_grid.astype(jnp.float32) + jnp.stack([step_y, step_x])


def transform(offsets, table, height, width):
    flat = offsets.reshape(2, -1)
    coef = jnp.dot(flat, table.T, precision=lax.Precision.HIGHEST)
    return jnp.eye(2, dtype=jnp.float32) + jnp.stack([coef[:, 0] / height, coef[:, 1] / width], axis=1)


def reference(sections, peaks):
    count, height, width = sections.shape
    pgy = height // PATCH
    pgx = width // PATCH
    margin = MAXOFF + 1
    table = jnp.asarray(fit_table(pgy, pgx, PATCH, height, width), jnp.float32)

    def pair(index):
        current = sections[index].astype(jnp.float32)
        before = jnp.where(index > 0, sections[jnp.maximum(index - 1, 0)].astype(jnp.float32), 0.0)
        padded = jnp.pad(before, margin)
        grid = peaks[index]
        rows_out = []
        errors_rows = []
        for i in range(pgy):
            cols_out = []
            errors_cols = []
            for j in range(pgx):
                start_y = (i * PATCH + margin - 1 + grid[0, i, j]).astype(jnp.int32)
                start_x = (j * PATCH + margin - 1 + grid[1, i, j]).astype(jnp.int32)
                window = lax.dynamic_slice(padded, (start_y, start_x), (PATCH + 2, PATCH + 2))
                piece = current[i * PATCH:(i + 1) * PATCH, j * PATCH:(j + 1) * PATCH]
                sums, error = moments(piece, window)
                cols_out.append(sums)
                errors_cols.append(error)
            rows_out.append(jnp.stack(cols_out, axis=1))
            errors_rows.append(jnp.concatenate(errors_cols, axis=1))
        sums = jnp.stack(rows_out, axis=1)
        image = jnp.concatenate(errors_rows, axis=0).astype(jnp.bfloat16)
        return solve_pairs(sums, grid), image

    offsets, residual = lax.map(pair, jnp.arange(count))

    def advance(carry, item):
        linear = transform(item, table, height, width)
        moved = jnp.dot(linear, carry, precision=lax.Precision.HIGHEST) + item.reshape(2, -1)
        return moved, moved

    _, cumulative = lax.scan(advance, jnp.zeros((2, pgy * pgx), jnp.float32), offsets)
    along_rows = spread(height, PATCH, pgy, 0)
    along_cols = spread(width, PATCH, pgx, 0)

    def dense(nodes):
        grid = nodes.reshape(2, pgy, pgx)
        wide = jnp.einsum('kij,cj->kic', grid, along_cols, precision=lax.Precision.HIGHEST)
        return jnp.einsum('ri,kic->krc', along_rows, wide, precision=lax.Precision.HIGHEST)

    field = lax.map(dense, cumulative)
    return field, offsets, residual
```

```python
import functools

import jax
import jax.numpy as jnp
import numpy as np
from jax import lax
from jax.experimental import pallas as pl
from jax.experimental.pallas import tpu as pltpu
from jax.sharding import PartitionSpec as P

PATCH = 1024
MAXOFF = 16
LAMBDA = 0.002
RIDGE = 0.05
EDGE = 32
SIDE = 128
BLOCK = 256
TILE = 64
MESH = pl.DeviceIdType.MESH


def invert_three(matrix):
    a, b, c = (matrix[0, 0], matrix[0, 1], matrix[0, 2])
    d, e, f = (matrix[1, 0], matrix[1, 1], matrix[1, 2])
    g, h, k = (matrix[2, 0], matrix[2, 1], matrix[2, 2])
    cof = np.array(
        [
            [e * k - f * h, c * h - b * k, b * f - c * e],
            [f * g - d * k, a * k - c * g, c * d - a * f],
            [d * h - e * g, b * g - a * h, a * e - b * d],
        ]
    )
    return cof / (a * (e * k - f * h) - b * (d * k - f * g) + c * (d * h - e * g))


def fit_table(pgy, pgx, patch, height, width):
    yy = ((np.arange(pgy) + 0.5) * patch - height / 2.0) / height
    xx = ((np.arange(pgx) + 0.5) * patch - width / 2.0) / width
    design = np.stack([np.repeat(yy, pgx), np.tile(xx, pgy), np.ones(pgy * pgx)], 1)
    ridge_matrix = np.array([[RIDGE, 0.0, 0.0], [0.0, RIDGE, 0.0], [0.0, 0.0, 0.0]])
    gram = design.T @ design + ridge_matrix
    return invert_three(gram) @ design.T


def register(G, R, pgy, pgx, table, peaks_hbm, sec, res, nodes, prev, cur, rmat, cmat, gmat, acc,
             gather, extra, peaks, peak_sem, cur_sem, ready, send_sem, recv_sem, rel_send, rel_recv,
             sum_send, sum_recv):
    band, width = sec.shape[1], sec.shape[2]
    height = band * R
    blocks = width // BLOCK
    per_patch = PATCH // BLOCK
    patches = pgy * pgx
    g, r = lax.axis_index("gz"), lax.axis_index("rows")
    f32, bf16 = jnp.float32, jnp.bfloat16

    spans = ((0, EDGE), (band - EDGE, EDGE), (EDGE, band - 2 * EDGE))

    def load(k):
        rows = pl.ds(*spans[k])
        return pltpu.make_async_copy(sec.at[0, rows, :], cur.at[rows, :], cur_sem.at[k])

    gather[...] = jnp.zeros_like(gather)
    barrier = pltpu.get_barrier_semaphore()

    @pl.when(g > 0)
    def _():
        pl.semaphore_signal(barrier, inc=1, device_id={"gz": g - 1}, device_id_type=MESH)

    for k in range(3):
        load(k).start()
    peak_load = pltpu.make_async_copy(peaks_hbm, peaks, peak_sem)
    peak_load.start()
    for d in range(1, R):
        pl.semaphore_signal(barrier, inc=1, device_id={"rows": lax.rem(r + d, R)}, device_id_type=MESH)

    @pl.when(g < G - 1)
    def _():
        pl.semaphore_signal(barrier, inc=1, device_id={"gz": g + 1}, device_id_type=MESH)

    pl.semaphore_wait(barrier, R - 1 + jnp.where(g > 0, 1, 0) + jnp.where(g < G - 1, 1, 0))
    rows_all = band + 2 * EDGE
    ahead = lax.rem(g + 1, G)

    def edge_copy(which):
        row = 0 if which == 0 else band - EDGE
        return pltpu.make_async_remote_copy(
            src_ref=cur.at[pl.ds(row, EDGE), :],
            dst_ref=prev.at[pl.ds(EDGE + row, EDGE), pl.ds(SIDE, width)],
            send_sem=send_sem.at[which], recv_sem=recv_sem.at[which],
            device_id={"gz": ahead}, device_id_type=MESH)

    def span_copy(k, col, count):
        return pltpu.make_async_remote_copy(
            src_ref=cur.at[pl.ds(EDGE, band - 2 * EDGE), pl.ds(col, count)],
            dst_ref=prev.at[pl.ds(2 * EDGE, band - 2 * EDGE), pl.ds(SIDE + col, count)],
            send_sem=send_sem.at[2 + k], recv_sem=recv_sem.at[2 + k],
            device_id={"gz": ahead}, device_id_type=MESH)

    def head_copy():
        return span_copy(0, 0, BLOCK + SIDE)

    def middle_copy(k):
        return span_copy(k, pl.multiple_of(k * BLOCK + SIDE, SIDE), BLOCK)

    def tail_copy():
        return span_copy(blocks - 1, width - BLOCK + SIDE, BLOCK - SIDE)

    def relay_up():
        return pltpu.make_async_remote_copy(
            src_ref=prev.at[pl.ds(EDGE, EDGE), pl.ds(SIDE, width)],
            dst_ref=prev.at[pl.ds(EDGE + band, EDGE), pl.ds(SIDE, width)],
            send_sem=rel_send.at[0], recv_sem=rel_recv.at[0],
            device_id={"rows": lax.rem(r + R - 1, R)}, device_id_type=MESH)

    def relay_down():
        return pltpu.make_async_remote_copy(
            src_ref=prev.at[pl.ds(band, EDGE), pl.ds(SIDE, width)],
            dst_ref=prev.at[pl.ds(0, EDGE), pl.ds(SIDE, width)],
            send_sem=rel_send.at[1], recv_sem=rel_recv.at[1],
            device_id={"rows": lax.rem(r + 1, R)}, device_id_type=MESH)

    for which in (0, 1):
        load(which).wait()

        @pl.when(g < G - 1)
        def _():
            edge_copy(which).start()

    load(2).wait()

    @pl.when(g < G - 1)
    def _():
        head_copy().start()
        lax.fori_loop(1, blocks - 1, lambda k, z: (middle_copy(k).start(), z)[1], 0)
        tail_copy().start()

    prev[:, 0:SIDE] = jnp.zeros((rows_all, SIDE), bf16)
    prev[:, SIDE + width :] = jnp.zeros((rows_all, SIDE), bf16)

    @pl.when(r == 0)
    def _():
        prev[0:EDGE, :] = jnp.zeros((EDGE, width + 2 * SIDE), bf16)

    @pl.when(r == R - 1)
    def _():
        prev[EDGE + band :, :] = jnp.zeros((EDGE, width + 2 * SIDE), bf16)

    @pl.when(g == 0)
    def _():
        def clear(t, z):
            prev[pl.ds(pl.multiple_of(t * EDGE, EDGE), EDGE), :] = jnp.zeros((EDGE, width + 2 * SIDE), bf16)
            return z

        lax.fori_loop(0, rows_all // EDGE, clear, 0)

    patch_row = r * band // PATCH
    peak_load.wait()
    rr = lax.broadcasted_iota(jnp.int32, (TILE, TILE + 2 * EDGE), 0)
    rk = lax.broadcasted_iota(jnp.int32, (TILE, TILE + 2 * EDGE), 1)
    ck = lax.broadcasted_iota(jnp.int32, (BLOCK + 2 * SIDE, BLOCK), 0)
    cn = lax.broadcasted_iota(jnp.int32, (BLOCK + 2 * SIDE, BLOCK), 1)
    rdiff = rk - rr - EDGE
    cdiff = ck - cn - SIDE
    for j in range(pgx):
        a = peaks[0, 0, patch_row, j]
        b = peaks[0, 1, patch_row, j]
        for n, step in enumerate((0, 1, -1)):
            rmat[j, n * TILE : (n + 1) * TILE, :] = jnp.where(rdiff == a + step, 1.0, 0.0).astype(bf16)
        cmat[j] = jnp.where(cdiff == b, 1.0, 0.0).astype(bf16)
        gmat[j] = jnp.where(cdiff == b + 1, 0.5, jnp.where(cdiff == b - 1, -0.5, 0.0)).astype(bf16)
    acc[...] = jnp.zeros_like(acc)

    lane = lax.broadcasted_iota(jnp.int32, (1, 128), 1)
    own_peaks = jnp.zeros((1, 128), f32)
    for i in range(pgy):
        for j in range(pgx):
            p = i * pgx + j
            own_peaks = jnp.where(lane == 5 * patches + p, peaks[0, 0, i, j].astype(f32), own_peaks)
            own_peaks = jnp.where(lane == 6 * patches + p, peaks[0, 1, i, j].astype(f32), own_peaks)
    extra[...] = jnp.where(r == 0, own_peaks, jnp.zeros((1, 128), f32))

    @pl.when(g < G - 1)
    def _():
        pl.semaphore_wait(ready, 1)

    @pl.when(g > 0)
    def _():
        pl.semaphore_signal(ready, inc=1, device_id={"gz": g - 1}, device_id_type=MESH)
        edge_copy(0).wait_recv()

        @pl.when(r > 0)
        def _():
            relay_up().start()

        edge_copy(1).wait_recv()

        @pl.when(r < R - 1)
        def _():
            relay_down().start()
            relay_up().wait_recv()

        @pl.when(r > 0)
        def _():
            relay_down().wait_recv()

        head_copy().wait_recv()

    tiles = band // TILE

    def fold(value):
        value = jnp.sum(value.reshape(value.shape[0] // 8, 8, BLOCK), axis=0)
        return sum(value[:, q : q + 128] for q in range(0, BLOCK, 128))

    def body(c, z):
        @pl.when((g > 0) & (c > 0) & (c < blocks - 1))
        def _():
            middle_copy(c).wait_recv()

        @pl.when((g > 0) & (c == blocks - 1))
        def _():
            tail_copy().wait_recv()

        j = c // per_patch
        col = pl.multiple_of(c * BLOCK, BLOCK)
        moved = []
        for t in range(tiles):
            window = prev[t * TILE : t * TILE + TILE + 2 * EDGE, pl.ds(col, BLOCK + 2 * SIDE)]
            moved.append(jnp.dot(rmat[j], window, preferred_element_type=f32).astype(bf16))
        parts = [jnp.concatenate([m[n * TILE : (n + 1) * TILE] for m in moved], axis=0) for n in range(3)]
        q = jnp.dot(parts[0], cmat[j], preferred_element_type=f32)
        lower = jnp.dot(parts[1], cmat[j], preferred_element_type=f32)
        upper = jnp.dot(parts[2], cmat[j], preferred_element_type=f32)
        gx = jnp.dot(parts[0], gmat[j], preferred_element_type=f32)
        gy = (lower - upper) * 0.5
        e = cur[:, pl.ds(col, BLOCK)].astype(f32) - q
        res[0, :, pl.ds(col, BLOCK)] = e.astype(bf16)
        for m, value in enumerate((gy * gy, gy * gx, gx * gx, gy * e, gx * e)):
            at = pl.ds(pl.multiple_of((m * pgx + j) * 8, 8), 8)
            acc[at, :] = acc[at, :] + fold(value)
        return z

    lax.fori_loop(0, blocks, body, 0)

    count = acc.shape[0] // 8
    totals = acc[pl.ds(0, count, stride=8), :]
    for k in range(1, 8):
        totals = totals + acc[pl.ds(k, count, stride=8), :]
    totals = jnp.sum(totals, axis=1, keepdims=True)
    place = lax.broadcasted_iota(jnp.int32, (count, 128), 0)
    for m in range(1, 5):
        place = place + jnp.where(lax.broadcasted_iota(jnp.int32, (count, 128), 0) >= m * pgx, patches - pgx, 0)
    hit = lax.broadcasted_iota(jnp.int32, (count, 128), 1) == place + patch_row * pgx
    mine = jnp.sum(jnp.where(hit, totals, 0.0), axis=0, keepdims=True)
    gather[r, pl.ds(g, 1), :] = mine + extra[...]

    def sum_copy(d, k):
        return pltpu.make_async_remote_copy(
            src_ref=gather.at[r, pl.ds(g, 1), :], dst_ref=gather.at[r, pl.ds(g, 1), :],
            send_sem=sum_send.at[d * R + k], recv_sem=sum_recv.at[r * G + g],
            device_id={"gz": g + d, "rows": lax.rem(r + k, R)}, device_id_type=MESH)

    def sum_arrival(s, k):
        origin = lax.rem(r + k, R)
        return pltpu.make_async_remote_copy(
            src_ref=gather.at[origin, pl.ds(s, 1), :], dst_ref=gather.at[origin, pl.ds(s, 1), :],
            send_sem=sum_send.at[0], recv_sem=sum_recv.at[origin * G + s],
            device_id={"rows": lax.rem(r + 1, R)}, device_id_type=MESH)

    def send_sums(i, z):
        d = G - 1 - g - i
        for k in range(R):
            if k:
                sum_copy(d, k).start()
            else:
                @pl.when(d > 0)
                def _():
                    sum_copy(d, k).start()
        return z

    lax.fori_loop(0, G - g, send_sums, 0)

    @pl.when(g < G - 1)
    def _():
        edge_copy(0).wait_send()
        edge_copy(1).wait_send()
        head_copy().wait_send()
        lax.fori_loop(1, blocks - 1, lambda k, z: (middle_copy(k).wait_send(), z)[1], 0)
        tail_copy().wait_send()

    @pl.when((g > 0) & (r > 0))
    def _():
        relay_up().wait_send()

    @pl.when((g > 0) & (r < R - 1))
    def _():
        relay_down().wait_send()

    def settle_sums(d, z):
        for k in range(R):
            if k:
                sum_copy(d, k).wait_send()
            else:
                @pl.when(d > 0)
                def _():
                    sum_copy(d, k).wait_send()
        return z

    lax.fori_loop(0, G - g, settle_sums, 0)

    def await_sums(s, z):
        for k in range(R):
            if k:
                sum_arrival(s, k).wait_recv()
            else:
                @pl.when(s < g)
                def _():
                    sum_arrival(s, k).wait_recv()
        return z

    lax.fori_loop(0, g + 1, await_sums, 0)

    full = gather[0]
    for k in range(1, R):
        full = full + gather[k]

    def moment(m):
        return pltpu.roll(full, 128 - m * patches, 1)

    damping = LAMBDA * PATCH * PATCH
    first = full + damping
    cross = moment(1)
    second = moment(2) + damping
    pull_y = moment(3)
    pull_x = moment(4)
    det = first * second - cross * cross
    valid = lax.broadcasted_iota(jnp.int32, (G, 128), 1) < patches
    off_y = jnp.where(valid, moment(5) + (second * pull_y - cross * pull_x) / det, 0.0)
    off_x = jnp.where(valid, moment(6) + (first * pull_x - cross * pull_y) / det, 0.0)
    ty = jnp.zeros((1, 128), f32)
    tx = jnp.zeros((1, 128), f32)
    for p in range(patches):
        ty = jnp.where(lane == p, float(table[0, p]), ty)
        tx = jnp.where(lane == p, float(table[1, p]), tx)

    def lanes(value):
        return jnp.broadcast_to(jnp.sum(value, axis=1, keepdims=True), (G, 128))

    yy = 1.0 + lanes(off_y * ty) / height
    yx = lanes(off_y * tx) / width
    xy = lanes(off_x * ty) / height
    xx = 1.0 + lanes(off_x * tx) / width
    uy = jnp.zeros((1, 128), f32)
    ux = jnp.zeros((1, 128), f32)
    for s in range(G):
        at = slice(s, s + 1)
        step_y = yy[at] * uy + yx[at] * ux + off_y[at]
        step_x = xy[at] * uy + xx[at] * ux + off_x[at]
        uy = jnp.where(s <= g, step_y, uy)
        ux = jnp.where(s <= g, step_x, ux)
    chosen = lax.broadcasted_iota(jnp.int32, (G, 128), 0) == g
    nodes[0:1] = uy
    nodes[1:2] = ux
    nodes[2:3] = jnp.sum(jnp.where(chosen, off_y, 0.0), axis=0, keepdims=True)
    nodes[3:4] = jnp.sum(jnp.where(chosen, off_x, 0.0), axis=0, keepdims=True)
    nodes[4:8] = jnp.zeros((4, 128), f32)


def spread_out(pgy, pgx, start_ref, nodes, res_in, field, offsets, res_out, buf, out_sem, field_sem):
    band, width = field.shape[2], field.shape[3]
    f32 = jnp.float32
    put = pltpu.make_async_copy(res_in, res_out, out_sem)
    put.start()
    cols = (lax.broadcasted_iota(jnp.int32, (8, width), 1).astype(f32) + 0.5) / PATCH - 0.5
    cols = jnp.clip(cols, 0.0, pgx - 1.0)
    weights = [jnp.maximum(0.0, 1.0 - jnp.abs(cols - j)) for j in range(pgx)]
    part = 32
    copies = []
    for k in range(2):
        wide = []
        for i in range(pgy):
            line = jnp.zeros((8, width), f32)
            for j in range(pgx):
                p = i * pgx + j
                line = line + weights[j] * nodes[k : k + 1, p : p + 1]
            wide.append(line)
        for t in range(band // part):
            slot = 0 if pgy == 1 else t
            for q in range(0, part, 8) if pgy > 1 or t == 0 else ():
                if pgy == 1:
                    block = wide[0]
                else:
                    rows = lax.broadcasted_iota(jnp.int32, (8, 1), 0).astype(f32) + start_ref[0].astype(f32)
                    pos = jnp.clip((rows + (t * part + q + 0.5)) / PATCH - 0.5, 0.0, pgy - 1.0)
                    block = sum(jnp.maximum(0.0, 1.0 - jnp.abs(pos - i)) * wide[i] for i in range(pgy))
                buf[k, slot * part + q : slot * part + q + 8, :] = block
            copy = pltpu.make_async_copy(
                buf.at[k, pl.ds(slot * part, part), :], field.at[0, k, pl.ds(t * part, part), :],
                field_sem.at[len(copies)])
            copy.start()
            copies.append(copy)
    offsets[...] = nodes[2:4, 0 : pgy * pgx]
    put.wait()
    for copy in copies:
        copy.wait()


def per_device(G, R, sections, peaks):
    band, width = sections.shape[1:]
    height = band * R
    pgy, pgx = height // PATCH, width // PATCH
    blocks = width // BLOCK
    f32, bf16 = jnp.float32, jnp.bfloat16
    table = fit_table(pgy, pgx, PATCH, height, width).astype(np.float32)
    vmem = pl.BlockSpec(memory_space=pltpu.VMEM)
    smem = pl.BlockSpec(memory_space=pltpu.SMEM)
    anywhere = pl.BlockSpec(memory_space=pl.ANY)
    dma = pltpu.SemaphoreType.DMA
    padded = -(-5 * pgx // 8) * 8
    residual, nodes = pl.pallas_call(
        functools.partial(register, G, R, pgy, pgx, table),
        name="register",
        out_shape=(jax.ShapeDtypeStruct((1, band, width), bf16), jax.ShapeDtypeStruct((8, 128), f32)),
        in_specs=[anywhere, anywhere],
        out_specs=(vmem, vmem),
        scratch_shapes=[
            pltpu.VMEM((band + 2 * EDGE, width + 2 * SIDE), bf16),
            pltpu.VMEM((band, width), bf16),
            pltpu.VMEM((pgx, 3 * TILE, TILE + 2 * EDGE), bf16),
            pltpu.VMEM((pgx, BLOCK + 2 * SIDE, BLOCK), bf16),
            pltpu.VMEM((pgx, BLOCK + 2 * SIDE, BLOCK), bf16),
            pltpu.VMEM((8 * padded, 128), f32),
            pltpu.VMEM((R, G, 128), f32),
            pltpu.VMEM((1, 128), f32),
            pltpu.SMEM((1, 2, pgy, pgx), jnp.int32),
            dma, dma((3,)), pltpu.SemaphoreType.REGULAR, dma((blocks + 2,)), dma((blocks + 2,)), dma((2,)), dma((2,)),
            dma((G * R,)), dma((G * R,)),
        ],
        compiler_params=pltpu.CompilerParams(collective_id=0, has_side_effects=True, vmem_limit_bytes=20 * 2**20),
    )(peaks, sections)
    start = (lax.axis_index("rows") * band).astype(jnp.int32).reshape(1)
    field, offsets, residual = pl.pallas_call(
        functools.partial(spread_out, pgy, pgx),
        name="spread_out",
        out_shape=(
            jax.ShapeDtypeStruct((1, 2, band, width), f32),
            jax.ShapeDtypeStruct((2, pgy * pgx), f32),
            jax.ShapeDtypeStruct((1, band, width), bf16),
        ),
        in_specs=[smem, vmem, vmem],
        out_specs=(anywhere, vmem, anywhere),
        scratch_shapes=[pltpu.VMEM((2, 32 if pgy == 1 else band, width), f32), dma, dma((2 * (band // 32),))],
        compiler_params=pltpu.CompilerParams(vmem_limit_bytes=20 * 2**20),
    )(start, nodes, residual)
    return field, offsets.reshape(1, 2, pgy, pgx), residual


def solution(mesh):
    return jax.shard_map(
        functools.partial(per_device, mesh.shape["gz"], mesh.shape["rows"]),
        mesh=mesh,
        in_specs=(P("gz", "rows", None), P("gz", None, None, None)),
        out_specs=(P("gz", None, "rows", None), P("gz", None, None, None), P("gz", "rows", None)),
        check_vma=False,
    )
```

```python
import functools

import jax
import jax.numpy as jnp
import numpy as np
from jax import lax
from jax.experimental import pallas as pl
from jax.experimental.pallas import tpu as pltpu
from jax.sharding import PartitionSpec as P

PATCH = 1024
MAXOFF = 16
LAMBDA = 0.002
RIDGE = 0.05
EDGE = 32
SIDE = 128
BLOCK = 256
TILE = 64
GROUP = 4
MESH = pl.DeviceIdType.MESH


def invert_three(matrix):
    a, b, c = (matrix[0, 0], matrix[0, 1], matrix[0, 2])
    d, e, f = (matrix[1, 0], matrix[1, 1], matrix[1, 2])
    g, h, k = (matrix[2, 0], matrix[2, 1], matrix[2, 2])
    cof = np.array(
        [
            [e * k - f * h, c * h - b * k, b * f - c * e],
            [f * g - d * k, a * k - c * g, c * d - a * f],
            [d * h - e * g, b * g - a * h, a * e - b * d],
        ]
    )
    return cof / (a * (e * k - f * h) - b * (d * k - f * g) + c * (d * h - e * g))


def fit_table(pgy, pgx, patch, height, width):
    yy = ((np.arange(pgy) + 0.5) * patch - height / 2.0) / height
    xx = ((np.arange(pgx) + 0.5) * patch - width / 2.0) / width
    design = np.stack([np.repeat(yy, pgx), np.tile(xx, pgy), np.ones(pgy * pgx)], 1)
    ridge_matrix = np.array([[RIDGE, 0.0, 0.0], [0.0, RIDGE, 0.0], [0.0, 0.0, 0.0]])
    gram = design.T @ design + ridge_matrix
    return invert_three(gram) @ design.T


def register(G, R, pgy, pgx, table, peaks_hbm, sec, res, nodes, prev, cur, rmat, cmat, gmat, acc,
             gather, extra, peaks, peak_sem, cur_sem, ready, send_sem, recv_sem, rel_send, rel_recv,
             sum_send, sum_recv):
    band, width = sec.shape[1], sec.shape[2]
    height = band * R
    blocks = width // BLOCK
    per_patch = PATCH // BLOCK
    patches = pgy * pgx
    g, r = lax.axis_index("gz"), lax.axis_index("rows")
    f32, bf16 = jnp.float32, jnp.bfloat16

    spans = ((0, EDGE), (band - EDGE, EDGE), (EDGE, band - 2 * EDGE))

    def load(k):
        rows = pl.ds(*spans[k])
        return pltpu.make_async_copy(sec.at[0, rows, :], cur.at[rows, :], cur_sem.at[k])

    gather[...] = jnp.zeros_like(gather)
    barrier = pltpu.get_barrier_semaphore()

    @pl.when(g > 0)
    def _():
        pl.semaphore_signal(barrier, inc=1, device_id={"gz": g - 1}, device_id_type=MESH)

    for k in range(3):
        load(k).start()
    peak_load = pltpu.make_async_copy(peaks_hbm, peaks, peak_sem)
    peak_load.start()

    @pl.when(r < R - 1)
    def _():
        pl.semaphore_signal(barrier, inc=1, device_id={"rows": r + 1}, device_id_type=MESH)

    @pl.when(g < G - 1)
    def _():
        pl.semaphore_signal(barrier, inc=1, device_id={"gz": g + 1}, device_id_type=MESH)

    greets = [jnp.where(near, 1, 0) for near in (g > 0, g < G - 1, r > 0)]
    pl.semaphore_wait(barrier, sum(greets))
    rows_all = band + 2 * EDGE
    ahead = lax.rem(g + 1, G)

    def edge_copy(which):
        row = 0 if which == 0 else band - EDGE
        return pltpu.make_async_remote_copy(
            src_ref=cur.at[pl.ds(row, EDGE), :],
            dst_ref=prev.at[pl.ds(EDGE + row, EDGE), pl.ds(SIDE, width)],
            send_sem=send_sem.at[which], recv_sem=recv_sem.at[which],
            device_id={"gz": ahead}, device_id_type=MESH)

    def span_copy(k, col, count):
        return pltpu.make_async_remote_copy(
            src_ref=cur.at[pl.ds(EDGE, band - 2 * EDGE), pl.ds(col, count)],
            dst_ref=prev.at[pl.ds(2 * EDGE, band - 2 * EDGE), pl.ds(SIDE + col, count)],
            send_sem=send_sem.at[2 + k], recv_sem=recv_sem.at[2 + k],
            device_id={"gz": ahead}, device_id_type=MESH)

    def head_copy():
        return span_copy(0, 0, BLOCK + SIDE)

    grouped = (blocks - 4) // GROUP * GROUP

    def group_copy(n):
        k = n * GROUP + 1
        return span_copy(k, pl.multiple_of(k * BLOCK + SIDE, SIDE), GROUP * BLOCK)

    def middle_copy(k):
        return span_copy(k, pl.multiple_of(k * BLOCK + SIDE, SIDE), BLOCK)

    def each_middle(act):
        lax.fori_loop(0, grouped // GROUP, lambda n, z: (act(group_copy(n)), z)[1], 0)
        lax.fori_loop(grouped + 1, blocks - 1, lambda k, z: (act(middle_copy(k)), z)[1], 0)

    def tail_copy():
        return span_copy(blocks - 1, width - BLOCK + SIDE, BLOCK - SIDE)

    def relay_up():
        return pltpu.make_async_remote_copy(
            src_ref=prev.at[pl.ds(EDGE, EDGE), pl.ds(SIDE, width)],
            dst_ref=prev.at[pl.ds(EDGE + band, EDGE), pl.ds(SIDE, width)],
            send_sem=rel_send.at[0], recv_sem=rel_recv.at[0],
            device_id={"rows": lax.rem(r + R - 1, R)}, device_id_type=MESH)

    def relay_down():
        return pltpu.make_async_remote_copy(
            src_ref=prev.at[pl.ds(band, EDGE), pl.ds(SIDE, width)],
            dst_ref=prev.at[pl.ds(0, EDGE), pl.ds(SIDE, width)],
            send_sem=rel_send.at[1], recv_sem=rel_recv.at[1],
            device_id={"rows": lax.rem(r + 1, R)}, device_id_type=MESH)

    for which in (0, 1):
        load(which).wait()

        @pl.when(g < G - 1)
        def _():
            edge_copy(which).start()

    load(2).wait()

    @pl.when(g < G - 1)
    def _():
        head_copy().start()
        each_middle(lambda copy: copy.start())
        tail_copy().start()

    prev[:, 0:SIDE] = jnp.zeros((rows_all, SIDE), bf16)
    prev[:, SIDE + width :] = jnp.zeros((rows_all, SIDE), bf16)

    @pl.when(r == 0)
    def _():
        prev[0:EDGE, :] = jnp.zeros((EDGE, width + 2 * SIDE), bf16)

    @pl.when(r == R - 1)
    def _():
        prev[EDGE + band :, :] = jnp.zeros((EDGE, width + 2 * SIDE), bf16)

    @pl.when(g == 0)
    def _():
        def clear(t, z):
            prev[pl.ds(pl.multiple_of(t * EDGE, EDGE), EDGE), :] = jnp.zeros((EDGE, width + 2 * SIDE), bf16)
            return z

        lax.fori_loop(0, rows_all // EDGE, clear, 0)

    patch_row = r * band // PATCH
    peak_load.wait()
    rr = lax.broadcasted_iota(jnp.int32, (TILE, TILE + 2 * EDGE), 0)
    rk = lax.broadcasted_iota(jnp.int32, (TILE, TILE + 2 * EDGE), 1)
    ck = lax.broadcasted_iota(jnp.int32, (BLOCK + 2 * SIDE, BLOCK), 0)
    cn = lax.broadcasted_iota(jnp.int32, (BLOCK + 2 * SIDE, BLOCK), 1)
    rdiff = rk - rr - EDGE
    cdiff = ck - cn - SIDE
    for j in range(pgx):
        a = peaks[0, 0, patch_row, j]
        b = peaks[0, 1, patch_row, j]
        for n, step in enumerate((0, 1, -1)):
            rmat[j, n * TILE : (n + 1) * TILE, :] = jnp.where(rdiff == a + step, 1.0, 0.0).astype(bf16)
        cmat[j] = jnp.where(cdiff == b, 1.0, 0.0).astype(bf16)
        gmat[j] = jnp.where(cdiff == b + 1, 0.5, jnp.where(cdiff == b - 1, -0.5, 0.0)).astype(bf16)
    acc[...] = jnp.zeros_like(acc)

    lane = lax.broadcasted_iota(jnp.int32, (1, 128), 1)
    own_peaks = jnp.zeros((1, 128), f32)
    for i in range(pgy):
        for j in range(pgx):
            p = i * pgx + j
            own_peaks = jnp.where(lane == 5 * patches + p, peaks[0, 0, i, j].astype(f32), own_peaks)
            own_peaks = jnp.where(lane == 6 * patches + p, peaks[0, 1, i, j].astype(f32), own_peaks)
    extra[...] = jnp.where(r == 0, own_peaks, jnp.zeros((1, 128), f32))

    @pl.when(r < R - 1)
    def _():
        pl.semaphore_wait(ready.at[1], 1)

    @pl.when(r > 0)
    def _():
        pl.semaphore_signal(ready.at[1], inc=1, device_id={"rows": r - 1}, device_id_type=MESH)
        pl.semaphore_wait(ready.at[2], 1)

    @pl.when(r < R - 1)
    def _():
        pl.semaphore_signal(ready.at[2], inc=1, device_id={"rows": r + 1}, device_id_type=MESH)

    @pl.when(g < G - 1)
    def _():
        pl.semaphore_wait(ready.at[0], 1)

    @pl.when(g > 0)
    def _():
        pl.semaphore_signal(ready.at[0], inc=1, device_id={"gz": g - 1}, device_id_type=MESH)
        edge_copy(0).wait_recv()

        @pl.when(r > 0)
        def _():
            relay_up().start()

        edge_copy(1).wait_recv()

        @pl.when(r < R - 1)
        def _():
            relay_down().start()
            relay_up().wait_recv()

        @pl.when(r > 0)
        def _():
            relay_down().wait_recv()

        head_copy().wait_recv()

    tiles = band // TILE

    def fold(value):
        value = jnp.sum(value.reshape(value.shape[0] // 8, 8, BLOCK), axis=0)
        return sum(value[:, q : q + 128] for q in range(0, BLOCK, 128))

    def body(c, z):
        @pl.when((g > 0) & (c % GROUP == 1) & (c <= grouped))
        def _():
            group_copy(c // GROUP).wait_recv()

        @pl.when((g > 0) & (c > grouped) & (c < blocks - 1))
        def _():
            middle_copy(c).wait_recv()

        @pl.when((g > 0) & (c == blocks - 1))
        def _():
            tail_copy().wait_recv()

        j = c // per_patch
        col = pl.multiple_of(c * BLOCK, BLOCK)
        moved = []
        for t in range(tiles):
            window = prev[t * TILE : t * TILE + TILE + 2 * EDGE, pl.ds(col, BLOCK + 2 * SIDE)]
            moved.append(jnp.dot(rmat[j], window, preferred_element_type=f32).astype(bf16))
        parts = [jnp.concatenate([m[n * TILE : (n + 1) * TILE] for m in moved], axis=0) for n in range(3)]
        q = jnp.dot(parts[0], cmat[j], preferred_element_type=f32)
        lower = jnp.dot(parts[1], cmat[j], preferred_element_type=f32)
        upper = jnp.dot(parts[2], cmat[j], preferred_element_type=f32)
        gx = jnp.dot(parts[0], gmat[j], preferred_element_type=f32)
        gy = (lower - upper) * 0.5
        e = cur[:, pl.ds(col, BLOCK)].astype(f32) - q
        res[0, :, pl.ds(col, BLOCK)] = e.astype(bf16)
        for m, value in enumerate((gy * gy, gy * gx, gx * gx, gy * e, gx * e)):
            at = pl.ds(pl.multiple_of((m * pgx + j) * 8, 8), 8)
            acc[at, :] = acc[at, :] + fold(value)
        return z

    lax.fori_loop(0, blocks, body, 0)

    count = acc.shape[0] // 8
    totals = acc[pl.ds(0, count, stride=8), :]
    for k in range(1, 8):
        totals = totals + acc[pl.ds(k, count, stride=8), :]
    totals = jnp.sum(totals, axis=1, keepdims=True)
    place = lax.broadcasted_iota(jnp.int32, (count, 128), 0)
    for m in range(1, 5):
        place = place + jnp.where(lax.broadcasted_iota(jnp.int32, (count, 128), 0) >= m * pgx, patches - pgx, 0)
    hit = lax.broadcasted_iota(jnp.int32, (count, 128), 1) == place + patch_row * pgx
    mine = jnp.sum(jnp.where(hit, totals, 0.0), axis=0, keepdims=True)
    gather[r, pl.ds(g, 1), :] = mine + extra[...]

    def sum_copy(d, k):
        return pltpu.make_async_remote_copy(
            src_ref=gather.at[r, pl.ds(g, 1), :], dst_ref=gather.at[r, pl.ds(g, 1), :],
            send_sem=sum_send.at[d * R + k], recv_sem=sum_recv.at[r * G + g],
            device_id={"gz": g + d, "rows": lax.rem(r + k, R)}, device_id_type=MESH)

    def sum_arrival(s, k):
        origin = lax.rem(r + k, R)
        return pltpu.make_async_remote_copy(
            src_ref=gather.at[origin, pl.ds(s, 1), :], dst_ref=gather.at[origin, pl.ds(s, 1), :],
            send_sem=sum_send.at[0], recv_sem=sum_recv.at[origin * G + s],
            device_id={"rows": lax.rem(r + 1, R)}, device_id_type=MESH)

    def send_sums(i, z):
        d = i
        for k in range(R):
            if k:
                sum_copy(d, k).start()
            else:
                @pl.when(d > 0)
                def _():
                    sum_copy(d, k).start()
        return z

    lax.fori_loop(0, G - g, send_sums, 0)

    @pl.when(g < G - 1)
    def _():
        edge_copy(0).wait_send()
        edge_copy(1).wait_send()
        head_copy().wait_send()
        each_middle(lambda copy: copy.wait_send())
        tail_copy().wait_send()

    @pl.when((g > 0) & (r > 0))
    def _():
        relay_up().wait_send()

    @pl.when((g > 0) & (r < R - 1))
    def _():
        relay_down().wait_send()

    def settle_sums(d, z):
        for k in range(R):
            if k:
                sum_copy(d, k).wait_send()
            else:
                @pl.when(d > 0)
                def _():
                    sum_copy(d, k).wait_send()
        return z

    lax.fori_loop(0, G - g, settle_sums, 0)

    def await_sums(s, z):
        for k in range(R):
            if k:
                sum_arrival(s, k).wait_recv()
            else:
                @pl.when(s < g)
                def _():
                    sum_arrival(s, k).wait_recv()
        return z

    lax.fori_loop(0, g + 1, await_sums, 0)

    full = gather[0]
    for k in range(1, R):
        full = full + gather[k]

    def moment(m):
        return pltpu.roll(full, 128 - m * patches, 1)

    damping = LAMBDA * PATCH * PATCH
    first = full + damping
    cross = moment(1)
    second = moment(2) + damping
    pull_y = moment(3)
    pull_x = moment(4)
    det = first * second - cross * cross
    valid = lax.broadcasted_iota(jnp.int32, (G, 128), 1) < patches
    off_y = jnp.where(valid, moment(5) + (second * pull_y - cross * pull_x) / det, 0.0)
    off_x = jnp.where(valid, moment(6) + (first * pull_x - cross * pull_y) / det, 0.0)
    ty = jnp.zeros((1, 128), f32)
    tx = jnp.zeros((1, 128), f32)
    for p in range(patches):
        ty = jnp.where(lane == p, float(table[0, p]), ty)
        tx = jnp.where(lane == p, float(table[1, p]), tx)

    def lanes(value):
        return jnp.broadcast_to(jnp.sum(value, axis=1, keepdims=True), (G, 128))

    yy = 1.0 + lanes(off_y * ty) / height
    yx = lanes(off_y * tx) / width
    xy = lanes(off_x * ty) / height
    xx = 1.0 + lanes(off_x * tx) / width
    uy = jnp.zeros((1, 128), f32)
    ux = jnp.zeros((1, 128), f32)
    for s in range(G):
        at = slice(s, s + 1)
        step_y = yy[at] * uy + yx[at] * ux + off_y[at]
        step_x = xy[at] * uy + xx[at] * ux + off_x[at]
        uy = jnp.where(s <= g, step_y, uy)
        ux = jnp.where(s <= g, step_x, ux)
    chosen = lax.broadcasted_iota(jnp.int32, (G, 128), 0) == g
    nodes[0:1] = uy
    nodes[1:2] = ux
    nodes[2:3] = jnp.sum(jnp.where(chosen, off_y, 0.0), axis=0, keepdims=True)
    nodes[3:4] = jnp.sum(jnp.where(chosen, off_x, 0.0), axis=0, keepdims=True)
    nodes[4:8] = jnp.zeros((4, 128), f32)


def spread_out(pgy, pgx, start_ref, nodes, res_in, field, offsets, res_out, buf, out_sem, field_sem):
    band, width = field.shape[2], field.shape[3]
    f32 = jnp.float32
    put = pltpu.make_async_copy(res_in, res_out, out_sem)
    put.start()
    cols = (lax.broadcasted_iota(jnp.int32, (8, width), 1).astype(f32) + 0.5) / PATCH - 0.5
    cols = jnp.clip(cols, 0.0, pgx - 1.0)
    weights = [jnp.maximum(0.0, 1.0 - jnp.abs(cols - j)) for j in range(pgx)]
    part = 32
    copies = []
    for k in range(2):
        wide = []
        for i in range(pgy):
            line = jnp.zeros((8, width), f32)
            for j in range(pgx):
                p = i * pgx + j
                line = line + weights[j] * nodes[k : k + 1, p : p + 1]
            wide.append(line)
        for t in range(band // part):
            slot = 0 if pgy == 1 else t
            for q in range(0, part, 8) if pgy > 1 or t == 0 else ():
                if pgy == 1:
                    block = wide[0]
                else:
                    rows = lax.broadcasted_iota(jnp.int32, (8, 1), 0).astype(f32) + start_ref[0].astype(f32)
                    pos = jnp.clip((rows + (t * part + q + 0.5)) / PATCH - 0.5, 0.0, pgy - 1.0)
                    block = sum(jnp.maximum(0.0, 1.0 - jnp.abs(pos - i)) * wide[i] for i in range(pgy))
                buf[k, slot * part + q : slot * part + q + 8, :] = block
            copy = pltpu.make_async_copy(
                buf.at[k, pl.ds(slot * part, part), :], field.at[0, k, pl.ds(t * part, part), :],
                field_sem.at[len(copies)])
            copy.start()
            copies.append(copy)
    offsets[...] = nodes[2:4, 0 : pgy * pgx]
    put.wait()
    for copy in copies:
        copy.wait()


def per_device(G, R, sections, peaks):
    band, width = sections.shape[1:]
    height = band * R
    pgy, pgx = height // PATCH, width // PATCH
    blocks = width // BLOCK
    f32, bf16 = jnp.float32, jnp.bfloat16
    table = fit_table(pgy, pgx, PATCH, height, width).astype(np.float32)
    vmem = pl.BlockSpec(memory_space=pltpu.VMEM)
    smem = pl.BlockSpec(memory_space=pltpu.SMEM)
    anywhere = pl.BlockSpec(memory_space=pl.ANY)
    dma = pltpu.SemaphoreType.DMA
    padded = -(-5 * pgx // 8) * 8
    residual, nodes = pl.pallas_call(
        functools.partial(register, G, R, pgy, pgx, table),
        name="register",
        out_shape=(jax.ShapeDtypeStruct((1, band, width), bf16), jax.ShapeDtypeStruct((8, 128), f32)),
        in_specs=[anywhere, anywhere],
        out_specs=(vmem, vmem),
        scratch_shapes=[
            pltpu.VMEM((band + 2 * EDGE, width + 2 * SIDE), bf16),
            pltpu.VMEM((band, width), bf16),
            pltpu.VMEM((pgx, 3 * TILE, TILE + 2 * EDGE), bf16),
            pltpu.VMEM((pgx, BLOCK + 2 * SIDE, BLOCK), bf16),
            pltpu.VMEM((pgx, BLOCK + 2 * SIDE, BLOCK), bf16),
            pltpu.VMEM((8 * padded, 128), f32),
            pltpu.VMEM((R, G, 128), f32),
            pltpu.VMEM((1, 128), f32),
            pltpu.SMEM((1, 2, pgy, pgx), jnp.int32),
            dma, dma((3,)), pltpu.SemaphoreType.REGULAR((3,)), dma((blocks + 2,)), dma((blocks + 2,)), dma((2,)), dma((2,)),
            dma((G * R,)), dma((G * R,)),
        ],
        compiler_params=pltpu.CompilerParams(collective_id=0, has_side_effects=True, vmem_limit_bytes=20 * 2**20),
    )(pltpu.with_memory_space_constraint(peaks, pltpu.HBM), pltpu.with_memory_space_constraint(sections, pltpu.HBM))
    start = (lax.axis_index("rows") * band).astype(jnp.int32).reshape(1)
    field, offsets, residual = pl.pallas_call(
        functools.partial(spread_out, pgy, pgx),
        name="spread_out",
        out_shape=(
            jax.ShapeDtypeStruct((1, 2, band, width), f32),
            jax.ShapeDtypeStruct((2, pgy * pgx), f32),
            jax.ShapeDtypeStruct((1, band, width), bf16),
        ),
        in_specs=[smem, vmem, vmem],
        out_specs=(anywhere, vmem, anywhere),
        scratch_shapes=[pltpu.VMEM((2, 32 if pgy == 1 else band, width), f32), dma, dma((2 * (band // 32),))],
        compiler_params=pltpu.CompilerParams(vmem_limit_bytes=20 * 2**20),
    )(start, nodes, residual)
    return field, offsets.reshape(1, 2, pgy, pgx), residual


def solution(mesh):
    return jax.shard_map(
        functools.partial(per_device, mesh.shape["gz"], mesh.shape["rows"]),
        mesh=mesh,
        in_specs=(P("gz", "rows", None), P("gz", None, None, None)),
        out_specs=(P("gz", None, "rows", None), P("gz", None, None, None), P("gz", "rows", None)),
        check_vma=False,
    )
```

```python
import functools

import jax
import jax.numpy as jnp
import numpy as np
from jax import lax
from jax.experimental import pallas as pl
from jax.experimental.pallas import tpu as pltpu
from jax.sharding import PartitionSpec as P

PATCH = 1024
MAXOFF = 16
LAMBDA = 0.002
RIDGE = 0.05
EDGE = 32
SIDE = 128
BLOCK = 256
GROUP = 4
MESH = pl.DeviceIdType.MESH


def invert_three(matrix):
    a, b, c = (matrix[0, 0], matrix[0, 1], matrix[0, 2])
    d, e, f = (matrix[1, 0], matrix[1, 1], matrix[1, 2])
    g, h, k = (matrix[2, 0], matrix[2, 1], matrix[2, 2])
    cof = np.array(
        [
            [e * k - f * h, c * h - b * k, b * f - c * e],
            [f * g - d * k, a * k - c * g, c * d - a * f],
            [d * h - e * g, b * g - a * h, a * e - b * d],
        ]
    )
    return cof / (a * (e * k - f * h) - b * (d * k - f * g) + c * (d * h - e * g))


def fit_table(pgy, pgx, patch, height, width):
    yy = ((np.arange(pgy) + 0.5) * patch - height / 2.0) / height
    xx = ((np.arange(pgx) + 0.5) * patch - width / 2.0) / width
    design = np.stack([np.repeat(yy, pgx), np.tile(xx, pgy), np.ones(pgy * pgx)], 1)
    ridge_matrix = np.array([[RIDGE, 0.0, 0.0], [0.0, RIDGE, 0.0], [0.0, 0.0, 0.0]])
    gram = design.T @ design + ridge_matrix
    return invert_three(gram) @ design.T


def register(G, R, pgy, pgx, table, peaks_hbm, sec, res, nodes, prev, cur, cmat, gmat, shifted, sloped, acc,
             gather, extra, peaks, peak_sem, cur_sem, ready, send_sem, recv_sem, rel_send, rel_recv,
             sum_send, sum_recv):
    band, width = sec.shape[1], sec.shape[2]
    height = band * R
    blocks = width // BLOCK
    per_patch = PATCH // BLOCK
    patches = pgy * pgx
    g, r = lax.axis_index("gz"), lax.axis_index("rows")
    f32, bf16 = jnp.float32, jnp.bfloat16

    spans = ((0, EDGE), (band - EDGE, EDGE), (EDGE, band - 2 * EDGE))

    def load(k):
        rows = pl.ds(*spans[k])
        return pltpu.make_async_copy(sec.at[0, rows, :], cur.at[rows, :], cur_sem.at[k])

    gather[...] = jnp.zeros_like(gather)
    barrier = pltpu.get_barrier_semaphore()

    @pl.when(g > 0)
    def _():
        pl.semaphore_signal(barrier, inc=1, device_id={"gz": g - 1}, device_id_type=MESH)

    for k in range(3):
        load(k).start()
    peak_load = pltpu.make_async_copy(peaks_hbm, peaks, peak_sem)
    peak_load.start()

    @pl.when(r < R - 1)
    def _():
        pl.semaphore_signal(barrier, inc=1, device_id={"rows": r + 1}, device_id_type=MESH)

    @pl.when(g < G - 1)
    def _():
        pl.semaphore_signal(barrier, inc=1, device_id={"gz": g + 1}, device_id_type=MESH)

    greets = [jnp.where(near, 1, 0) for near in (g > 0, g < G - 1, r > 0)]
    pl.semaphore_wait(barrier, sum(greets))
    rows_all = band + 2 * EDGE
    ahead = lax.rem(g + 1, G)

    def edge_copy(which):
        row = 0 if which == 0 else band - EDGE
        return pltpu.make_async_remote_copy(
            src_ref=cur.at[pl.ds(row, EDGE), :],
            dst_ref=prev.at[pl.ds(EDGE + row, EDGE), pl.ds(SIDE, width)],
            send_sem=send_sem, recv_sem=recv_sem.at[which],
            device_id={"gz": ahead}, device_id_type=MESH)

    def span_copy(index, col, count):
        return pltpu.make_async_remote_copy(
            src_ref=cur.at[pl.ds(EDGE, band - 2 * EDGE), pl.ds(col, count)],
            dst_ref=prev.at[pl.ds(2 * EDGE, band - 2 * EDGE), pl.ds(SIDE + col, count)],
            send_sem=send_sem, recv_sem=recv_sem.at[2 + index],
            device_id={"gz": ahead}, device_id_type=MESH)

    def head_copy():
        return span_copy(0, 0, BLOCK + SIDE)

    grouped = (blocks - 4) // GROUP * GROUP
    singles = grouped // GROUP - grouped

    def group_copy(n):
        k = n * GROUP + 1
        return span_copy(1 + n, pl.multiple_of(k * BLOCK + SIDE, SIDE), GROUP * BLOCK)

    def middle_copy(k):
        return span_copy(singles + k, pl.multiple_of(k * BLOCK + SIDE, SIDE), BLOCK)

    def tail_copy():
        return span_copy(singles + blocks - 1, width - BLOCK + SIDE, BLOCK - SIDE)

    def relay_up():
        return pltpu.make_async_remote_copy(
            src_ref=prev.at[pl.ds(EDGE, EDGE), pl.ds(SIDE, width)],
            dst_ref=prev.at[pl.ds(EDGE + band, EDGE), pl.ds(SIDE, width)],
            send_sem=rel_send.at[0], recv_sem=rel_recv.at[0],
            device_id={"rows": lax.rem(r + R - 1, R)}, device_id_type=MESH)

    def relay_down():
        return pltpu.make_async_remote_copy(
            src_ref=prev.at[pl.ds(band, EDGE), pl.ds(SIDE, width)],
            dst_ref=prev.at[pl.ds(0, EDGE), pl.ds(SIDE, width)],
            send_sem=rel_send.at[1], recv_sem=rel_recv.at[1],
            device_id={"rows": lax.rem(r + 1, R)}, device_id_type=MESH)

    for which in (0, 1):
        load(which).wait()

        @pl.when(g < G - 1)
        def _():
            edge_copy(which).start()

    load(2).wait()

    @pl.when(g < G - 1)
    def _():
        head_copy().start()
        lax.fori_loop(0, grouped // GROUP, lambda n, z: (group_copy(n).start(), z)[1], 0)
        lax.fori_loop(grouped + 1, blocks - 1, lambda k, z: (middle_copy(k).start(), z)[1], 0)
        tail_copy().start()

    prev[:, 0:SIDE] = jnp.zeros((rows_all, SIDE), bf16)
    prev[:, SIDE + width :] = jnp.zeros((rows_all, SIDE), bf16)

    @pl.when(r == 0)
    def _():
        prev[0:EDGE, :] = jnp.zeros((EDGE, width + 2 * SIDE), bf16)

    @pl.when(r == R - 1)
    def _():
        prev[EDGE + band :, :] = jnp.zeros((EDGE, width + 2 * SIDE), bf16)

    @pl.when(g == 0)
    def _():
        def clear(t, z):
            prev[pl.ds(pl.multiple_of(t * EDGE, EDGE), EDGE), :] = jnp.zeros((EDGE, width + 2 * SIDE), bf16)
            return z

        lax.fori_loop(0, rows_all // EDGE, clear, 0)

    patch_row = r * band // PATCH
    peak_load.wait()
    ck = lax.broadcasted_iota(jnp.int32, (BLOCK + 2 * SIDE, BLOCK), 0)
    cn = lax.broadcasted_iota(jnp.int32, (BLOCK + 2 * SIDE, BLOCK), 1)
    cdiff = ck - cn - SIDE

    def build(j, z):
        b = peaks[0, 1, patch_row, j]
        cmat[j] = jnp.where(cdiff == b, 1.0, 0.0).astype(bf16)
        gmat[j] = jnp.where(cdiff == b + 1, 0.5, jnp.where(cdiff == b - 1, -0.5, 0.0)).astype(bf16)
        return z

    lax.fori_loop(0, pgx, build, 0)
    acc[...] = jnp.zeros_like(acc)

    lane = lax.broadcasted_iota(jnp.int32, (1, 128), 1)
    own_peaks = jnp.zeros((1, 128), f32)
    for i in range(pgy):
        for j in range(pgx):
            p = i * pgx + j
            own_peaks = jnp.where(lane == 5 * patches + p, peaks[0, 0, i, j].astype(f32), own_peaks)
            own_peaks = jnp.where(lane == 6 * patches + p, peaks[0, 1, i, j].astype(f32), own_peaks)
    extra[...] = jnp.where(r == 0, own_peaks, jnp.zeros((1, 128), f32))

    @pl.when(r < R - 1)
    def _():
        pl.semaphore_wait(ready.at[1], 1)

    @pl.when(r > 0)
    def _():
        pl.semaphore_signal(ready.at[1], inc=1, device_id={"rows": r - 1}, device_id_type=MESH)
        pl.semaphore_wait(ready.at[2], 1)

    @pl.when(r < R - 1)
    def _():
        pl.semaphore_signal(ready.at[2], inc=1, device_id={"rows": r + 1}, device_id_type=MESH)

    @pl.when(g < G - 1)
    def _():
        pl.semaphore_wait(ready.at[0], 1)

    @pl.when(g > 0)
    def _():
        pl.semaphore_signal(ready.at[0], inc=1, device_id={"gz": g - 1}, device_id_type=MESH)
        edge_copy(0).wait_recv()

        @pl.when(r > 0)
        def _():
            relay_up().start()

        edge_copy(1).wait_recv()

        @pl.when(r < R - 1)
        def _():
            relay_down().start()
            relay_up().wait_recv()

        @pl.when(r > 0)
        def _():
            relay_down().wait_recv()

        head_copy().wait_recv()

    def body(c, z):
        @pl.when((g > 0) & (c % GROUP == 1) & (c <= grouped))
        def _():
            group_copy(c // GROUP).wait_recv()

        @pl.when((g > 0) & (c > grouped) & (c < blocks - 1))
        def _():
            middle_copy(c).wait_recv()

        @pl.when((g > 0) & (c == blocks - 1))
        def _():
            tail_copy().wait_recv()

        j = c // per_patch
        col = pl.multiple_of(c * BLOCK, BLOCK)
        window = prev[:, pl.ds(col, BLOCK + 2 * SIDE)]
        moved = jnp.dot(window, cmat[j], preferred_element_type=f32)
        slope = jnp.dot(window, gmat[j], preferred_element_type=f32)
        down = EDGE + peaks[0, 0, patch_row, j]
        sums = [jnp.zeros((8, 128), f32) for _ in range(5)]
        for n in range(BLOCK // 128):
            shifted[n] = moved[:, n * 128 : (n + 1) * 128]
            sloped[n] = slope[:, n * 128 : (n + 1) * 128]
        for n in range(BLOCK // 128):
            q = shifted[n, pl.ds(down, band), :]
            gy = (shifted[n, pl.ds(down + 1, band), :] - shifted[n, pl.ds(down - 1, band), :]) * 0.5
            gx = sloped[n, pl.ds(down, band), :]
            e = cur[:, pl.ds(col + n * 128, 128)].astype(f32) - q
            res[0, :, pl.ds(col + n * 128, 128)] = e.astype(bf16)
            for m, value in enumerate((gy * gy, gy * gx, gx * gx, gy * e, gx * e)):
                sums[m] = sums[m] + jnp.sum(value.reshape(band // 8, 8, 128), axis=0)
        for m, value in enumerate(sums):
            at = pl.ds(pl.multiple_of((m * pgx + j) * 8, 8), 8)
            acc[at, :] = acc[at, :] + value
        return z

    lax.fori_loop(0, blocks, body, 0)

    count = acc.shape[0] // 8
    totals = acc[pl.ds(0, count, stride=8), :]
    for k in range(1, 8):
        totals = totals + acc[pl.ds(k, count, stride=8), :]
    totals = jnp.sum(totals, axis=1, keepdims=True)
    place = lax.broadcasted_iota(jnp.int32, (count, 128), 0)
    for m in range(1, 5):
        place = place + jnp.where(lax.broadcasted_iota(jnp.int32, (count, 128), 0) >= m * pgx, patches - pgx, 0)
    hit = lax.broadcasted_iota(jnp.int32, (count, 128), 1) == place + patch_row * pgx
    mine = jnp.sum(jnp.where(hit, totals, 0.0), axis=0, keepdims=True)
    slot = pl.ds(r * G + g, 1)
    gather[slot, :] = mine + extra[...]

    def sum_copy(d, k):
        return pltpu.make_async_remote_copy(
            src_ref=gather.at[slot], dst_ref=gather.at[slot], send_sem=sum_send, recv_sem=sum_recv,
            device_id={"gz": g + d, "rows": lax.rem(r + k, R)}, device_id_type=MESH)

    def all_sums(count):
        return pltpu.make_async_remote_copy(
            src_ref=gather.at[pl.ds(0, count)], dst_ref=gather.at[pl.ds(0, count)],
            send_sem=sum_send, recv_sem=sum_recv, device_id={"rows": lax.rem(r + 1, R)}, device_id_type=MESH)

    def send_sums(i, z):
        d = i
        for k in range(R):
            if k:
                sum_copy(d, k).start()
            else:
                @pl.when(d > 0)
                def _():
                    sum_copy(d, k).start()
        return z

    lax.fori_loop(0, G - g, send_sums, 0)

    @pl.when(g < G - 1)
    def _():
        pltpu.make_async_remote_copy(
            src_ref=cur, dst_ref=cur, send_sem=send_sem, recv_sem=recv_sem.at[0],
            device_id={"gz": ahead}, device_id_type=MESH).wait_send()

    @pl.when((g > 0) & (r > 0))
    def _():
        relay_up().wait_send()

    @pl.when((g > 0) & (r < R - 1))
    def _():
        relay_down().wait_send()

    for s in range(G):
        @pl.when(g == s)
        def _():
            all_sums(R * (G - s) - 1).wait_send()
            all_sums(R * (s + 1) - 1).wait_recv()

    full = gather[0:G]
    for k in range(1, R):
        full = full + gather[k * G : (k + 1) * G]

    def moment(m):
        return pltpu.roll(full, 128 - m * patches, 1)

    damping = LAMBDA * PATCH * PATCH
    first = full + damping
    cross = moment(1)
    second = moment(2) + damping
    pull_y = moment(3)
    pull_x = moment(4)
    det = first * second - cross * cross
    valid = lax.broadcasted_iota(jnp.int32, (G, 128), 1) < patches
    off_y = jnp.where(valid, moment(5) + (second * pull_y - cross * pull_x) / det, 0.0)
    off_x = jnp.where(valid, moment(6) + (first * pull_x - cross * pull_y) / det, 0.0)
    ty = jnp.zeros((1, 128), f32)
    tx = jnp.zeros((1, 128), f32)
    for p in range(patches):
        ty = jnp.where(lane == p, float(table[0, p]), ty)
        tx = jnp.where(lane == p, float(table[1, p]), tx)

    def lanes(value):
        return jnp.broadcast_to(jnp.sum(value, axis=1, keepdims=True), (G, 128))

    yy = 1.0 + lanes(off_y * ty) / height
    yx = lanes(off_y * tx) / width
    xy = lanes(off_x * ty) / height
    xx = 1.0 + lanes(off_x * tx) / width
    uy = jnp.zeros((1, 128), f32)
    ux = jnp.zeros((1, 128), f32)
    for s in range(G):
        at = slice(s, s + 1)
        step_y = yy[at] * uy + yx[at] * ux + off_y[at]
        step_x = xy[at] * uy + xx[at] * ux + off_x[at]
        uy = jnp.where(s <= g, step_y, uy)
        ux = jnp.where(s <= g, step_x, ux)
    chosen = lax.broadcasted_iota(jnp.int32, (G, 128), 0) == g
    nodes[0:1] = uy
    nodes[1:2] = ux
    nodes[2:3] = jnp.sum(jnp.where(chosen, off_y, 0.0), axis=0, keepdims=True)
    nodes[3:4] = jnp.sum(jnp.where(chosen, off_x, 0.0), axis=0, keepdims=True)
    nodes[4:8] = jnp.zeros((4, 128), f32)


def spread_out(pgy, pgx, nodes, res_in, field, offsets, res_out, buf, out_sem, field_sem):
    band, width = field.shape[2], field.shape[3]
    f32 = jnp.float32
    put = pltpu.make_async_copy(res_in, res_out, out_sem)
    put.start()
    cols = (lax.broadcasted_iota(jnp.int32, (8, width), 1).astype(f32) + 0.5) / PATCH - 0.5
    cols = jnp.clip(cols, 0.0, pgx - 1.0)
    weights = [jnp.maximum(0.0, 1.0 - jnp.abs(cols - j)) for j in range(pgx)]
    part = 32
    for k in range(2):
        wide = []
        for i in range(pgy):
            line = jnp.zeros((8, width), f32)
            for j in range(pgx):
                p = i * pgx + j
                line = line + weights[j] * nodes[k : k + 1, p : p + 1]
            wide.append(line)
        for t in range(band // part):
            slot = 0 if pgy == 1 else t
            for q in range(0, part, 8) if pgy > 1 or t == 0 else ():
                if pgy == 1:
                    block = wide[0]
                else:
                    rows = (lax.broadcasted_iota(jnp.int32, (8, 1), 0) + lax.axis_index("rows") * band).astype(f32)
                    pos = jnp.clip((rows + (t * part + q + 0.5)) / PATCH - 0.5, 0.0, pgy - 1.0)
                    block = sum(jnp.maximum(0.0, 1.0 - jnp.abs(pos - i)) * wide[i] for i in range(pgy))
                buf[k, slot * part + q : slot * part + q + 8, :] = block
            pltpu.make_async_copy(
                buf.at[k, pl.ds(slot * part, part), :], field.at[0, k, pl.ds(t * part, part), :], field_sem).start()
    offsets[...] = nodes[2:4, 0 : pgy * pgx]
    put.wait()
    pltpu.make_async_copy(field, field, field_sem).wait()


def per_device(G, R, sections, peaks):
    band, width = sections.shape[1:]
    height = band * R
    pgy, pgx = height // PATCH, width // PATCH
    blocks = width // BLOCK
    f32, bf16 = jnp.float32, jnp.bfloat16
    table = fit_table(pgy, pgx, PATCH, height, width).astype(np.float32)
    vmem = pl.BlockSpec(memory_space=pltpu.VMEM)
    anywhere = pl.BlockSpec(memory_space=pl.ANY)
    dma = pltpu.SemaphoreType.DMA
    padded = -(-5 * pgx // 8) * 8
    grouped = (blocks - 4) // GROUP * GROUP
    arrivals = 2 + blocks - grouped + grouped // GROUP
    residual, nodes = pl.pallas_call(
        functools.partial(register, G, R, pgy, pgx, table),
        name="register",
        out_shape=(jax.ShapeDtypeStruct((1, band, width), bf16), jax.ShapeDtypeStruct((8, 128), f32)),
        in_specs=[anywhere, anywhere],
        out_specs=(vmem, vmem),
        scratch_shapes=[
            pltpu.VMEM((band + 2 * EDGE, width + 2 * SIDE), bf16),
            pltpu.VMEM((band, width), bf16),
            pltpu.VMEM((pgx, BLOCK + 2 * SIDE, BLOCK), bf16),
            pltpu.VMEM((pgx, BLOCK + 2 * SIDE, BLOCK), bf16),
            pltpu.VMEM((BLOCK // 128, band + 2 * EDGE, 128), f32),
            pltpu.VMEM((BLOCK // 128, band + 2 * EDGE, 128), f32),
            pltpu.VMEM((8 * padded, 128), f32),
            pltpu.VMEM((R * G, 128), f32),
            pltpu.VMEM((1, 128), f32),
            pltpu.SMEM((1, 2, pgy, pgx), jnp.int32),
            dma, dma((3,)), pltpu.SemaphoreType.REGULAR((3,)), dma, dma((arrivals,)), dma((2,)), dma((2,)),
            dma, dma,
        ],
        compiler_params=pltpu.CompilerParams(collective_id=0, has_side_effects=True, vmem_limit_bytes=20 * 2**20),
    )(pltpu.with_memory_space_constraint(peaks, pltpu.HBM), pltpu.with_memory_space_constraint(sections, pltpu.HBM))
    field, offsets, residual = pl.pallas_call(
        functools.partial(spread_out, pgy, pgx),
        name="spread_out",
        out_shape=(
            jax.ShapeDtypeStruct((1, 2, band, width), f32),
            jax.ShapeDtypeStruct((2, pgy * pgx), f32),
            jax.ShapeDtypeStruct((1, band, width), bf16),
        ),
        in_specs=[vmem, vmem],
        out_specs=(anywhere, vmem, anywhere),
        scratch_shapes=[pltpu.VMEM((2, 32 if pgy == 1 else band, width), f32), dma, dma],
        compiler_params=pltpu.CompilerParams(vmem_limit_bytes=20 * 2**20),
    )(nodes, residual)
    return field, offsets.reshape(1, 2, pgy, pgx), residual


def solution(mesh):
    return jax.shard_map(
        functools.partial(per_device, mesh.shape["gz"], mesh.shape["rows"]),
        mesh=mesh,
        in_specs=(P("gz", "rows", None), P("gz", None, None, None)),
        out_specs=(P("gz", None, "rows", None), P("gz", None, None, None), P("gz", "rows", None)),
        check_vma=False,
    )
```

```python
import functools

import jax
import jax.numpy as jnp
import numpy as np
from jax import lax
from jax.experimental import pallas as pl
from jax.experimental.pallas import tpu as pltpu
from jax.sharding import PartitionSpec as P

PATCH = 1024
MAXOFF = 16
LAMBDA = 0.002
RIDGE = 0.05
EDGE = 32
SIDE = 128
BLOCK = 256
GROUP = 4
LATE = 2
MESH = pl.DeviceIdType.MESH


def invert_three(matrix):
    a, b, c = (matrix[0, 0], matrix[0, 1], matrix[0, 2])
    d, e, f = (matrix[1, 0], matrix[1, 1], matrix[1, 2])
    g, h, k = (matrix[2, 0], matrix[2, 1], matrix[2, 2])
    cof = np.array(
        [
            [e * k - f * h, c * h - b * k, b * f - c * e],
            [f * g - d * k, a * k - c * g, c * d - a * f],
            [d * h - e * g, b * g - a * h, a * e - b * d],
        ]
    )
    return cof / (a * (e * k - f * h) - b * (d * k - f * g) + c * (d * h - e * g))


def fit_table(pgy, pgx, patch, height, width):
    yy = ((np.arange(pgy) + 0.5) * patch - height / 2.0) / height
    xx = ((np.arange(pgx) + 0.5) * patch - width / 2.0) / width
    design = np.stack([np.repeat(yy, pgx), np.tile(xx, pgy), np.ones(pgy * pgx)], 1)
    ridge_matrix = np.array([[RIDGE, 0.0, 0.0], [0.0, RIDGE, 0.0], [0.0, 0.0, 0.0]])
    gram = design.T @ design + ridge_matrix
    return invert_three(gram) @ design.T


def register(G, R, pgy, pgx, table, peaks_hbm, sec, res, nodes, prev, cur, cmat, gmat, shifted, sloped, acc,
             gather, extra, peaks, peak_sem, cur_sem, ready, send_sem, recv_sem, rel_send, rel_recv,
             sum_send, sum_recv, late, shift_row, shifts, late_send, late_recv, shift_recv, rows_send, rows_recv, late_acc):
    band, width = sec.shape[1], sec.shape[2]
    height = band * R
    blocks = width // BLOCK
    per_patch = PATCH // BLOCK
    patches = pgy * pgx
    g, r = lax.axis_index("gz"), lax.axis_index("rows")
    f32, bf16 = jnp.float32, jnp.bfloat16

    spans = ((0, EDGE), (band - EDGE, EDGE), (EDGE, band - 2 * EDGE))

    def load(k):
        rows = pl.ds(*spans[k])
        return pltpu.make_async_copy(sec.at[0, rows, :], cur.at[rows, :], cur_sem.at[k])

    gather[...] = jnp.zeros_like(gather)
    barrier = pltpu.get_barrier_semaphore()

    @pl.when(g > 0)
    def _():
        pl.semaphore_signal(barrier, inc=1, device_id={"gz": g - 1}, device_id_type=MESH)

    for k in range(3):
        load(k).start()
    peak_load = pltpu.make_async_copy(peaks_hbm, peaks, peak_sem)
    peak_load.start()

    @pl.when(r < R - 1)
    def _():
        pl.semaphore_signal(barrier, inc=1, device_id={"rows": r + 1}, device_id_type=MESH)

    @pl.when(g < G - 1)
    def _():
        pl.semaphore_signal(barrier, inc=1, device_id={"gz": g + 1}, device_id_type=MESH)

    greets = [jnp.where(near, 1, 0) for near in (g > 0, g < G - 1, r > 0)]
    pl.semaphore_wait(barrier, sum(greets))
    rows_all = band + 2 * EDGE
    reach = LATE * BLOCK + SIDE
    ahead = lax.rem(g + 1, G)

    def edge_copy(which):
        row = 0 if which == 0 else band - EDGE
        return pltpu.make_async_remote_copy(
            src_ref=cur.at[pl.ds(row, EDGE), :],
            dst_ref=prev.at[pl.ds(EDGE + row, EDGE), pl.ds(SIDE, width)],
            send_sem=send_sem, recv_sem=recv_sem.at[which],
            device_id={"gz": ahead}, device_id_type=MESH)

    def span_copy(index, col, count):
        return pltpu.make_async_remote_copy(
            src_ref=cur.at[pl.ds(EDGE, band - 2 * EDGE), pl.ds(col, count)],
            dst_ref=prev.at[pl.ds(2 * EDGE, band - 2 * EDGE), pl.ds(SIDE + col, count)],
            send_sem=send_sem, recv_sem=recv_sem.at[2 + index],
            device_id={"gz": ahead}, device_id_type=MESH)

    def head_copy():
        return span_copy(0, 0, BLOCK + SIDE)

    grouped = (blocks - 4) // GROUP * GROUP
    singles = grouped // GROUP - grouped

    def group_copy(n):
        k = n * GROUP + 1
        return span_copy(1 + n, pl.multiple_of(k * BLOCK + SIDE, SIDE), GROUP * BLOCK)

    def middle_copy(k):
        return span_copy(singles + k, pl.multiple_of(k * BLOCK + SIDE, SIDE), BLOCK)

    def tail_copy():
        return span_copy(singles + blocks - 1, width - BLOCK + SIDE, BLOCK - SIDE)

    def relay_up():
        return pltpu.make_async_remote_copy(
            src_ref=prev.at[pl.ds(EDGE, EDGE), pl.ds(SIDE, width)],
            dst_ref=prev.at[pl.ds(EDGE + band, EDGE), pl.ds(SIDE, width)],
            send_sem=rel_send, recv_sem=rel_recv,
            device_id={"rows": lax.rem(r + R - 1, R)}, device_id_type=MESH)

    def relay_down():
        return pltpu.make_async_remote_copy(
            src_ref=prev.at[pl.ds(band, EDGE), pl.ds(SIDE, width)],
            dst_ref=prev.at[pl.ds(0, EDGE), pl.ds(SIDE, width)],
            send_sem=rel_send, recv_sem=rel_recv,
            device_id={"rows": lax.rem(r + 1, R)}, device_id_type=MESH)

    def both_relays(count):
        rows = pl.ds(0, count * EDGE)
        return pltpu.make_async_remote_copy(
            src_ref=cur.at[rows, :], dst_ref=cur.at[rows, :], send_sem=rel_send, recv_sem=rel_recv,
            device_id={"rows": lax.rem(r + 1, R)}, device_id_type=MESH)

    for which in (0, 1):
        load(which).wait()

        @pl.when(g < G - 1)
        def _():
            edge_copy(which).start()

    load(2).wait()

    @pl.when(g < G - 1)
    def _():
        head_copy().start()
        lax.fori_loop(0, grouped // GROUP, lambda n, z: (group_copy(n).start(), z)[1], 0)
        lax.fori_loop(grouped + 1, blocks - 1, lambda k, z: (middle_copy(k).start(), z)[1], 0)
        tail_copy().start()

    prev[:, 0:SIDE] = jnp.zeros((rows_all, SIDE), bf16)
    prev[:, SIDE + width :] = jnp.zeros((rows_all, SIDE), bf16)

    @pl.when(r == 0)
    def _():
        prev[0:EDGE, :] = jnp.zeros((EDGE, width + 2 * SIDE), bf16)

    @pl.when(r == R - 1)
    def _():
        prev[EDGE + band :, :] = jnp.zeros((EDGE, width + 2 * SIDE), bf16)

    @pl.when(g == 0)
    def _():
        def clear(t, z):
            prev[pl.ds(pl.multiple_of(t * EDGE, EDGE), EDGE), :] = jnp.zeros((EDGE, width + 2 * SIDE), bf16)
            return z

        lax.fori_loop(0, rows_all // EDGE, clear, 0)

    patch_row = r * band // PATCH
    peak_load.wait()
    ck = lax.broadcasted_iota(jnp.int32, (BLOCK + 2 * SIDE, BLOCK), 0)
    cn = lax.broadcasted_iota(jnp.int32, (BLOCK + 2 * SIDE, BLOCK), 1)
    cdiff = ck - cn - SIDE

    def build(j, z):
        b = peaks[0, 1, patch_row, j]
        cmat[j] = jnp.where(cdiff == b, 1.0, 0.0).astype(bf16)
        gmat[j] = jnp.where(cdiff == b + 1, 0.5, jnp.where(cdiff == b - 1, -0.5, 0.0)).astype(bf16)
        return z

    lax.fori_loop(0, pgx, build, 0)
    acc[...] = jnp.zeros_like(acc)

    lane = lax.broadcasted_iota(jnp.int32, (1, 128), 1)
    own_peaks = jnp.zeros((1, 128), f32)
    for i in range(pgy):
        for j in range(pgx):
            p = i * pgx + j
            own_peaks = jnp.where(lane == 5 * patches + p, peaks[0, 0, i, j].astype(f32), own_peaks)
            own_peaks = jnp.where(lane == 6 * patches + p, peaks[0, 1, i, j].astype(f32), own_peaks)
    extra[...] = jnp.where(r == 0, own_peaks, jnp.zeros((1, 128), f32))

    @pl.when(r < R - 1)
    def _():
        pl.semaphore_wait(ready.at[1], 1)

    @pl.when(r > 0)
    def _():
        pl.semaphore_signal(ready.at[1], inc=1, device_id={"rows": r - 1}, device_id_type=MESH)
        pl.semaphore_wait(ready.at[2], 1)

    @pl.when(r < R - 1)
    def _():
        pl.semaphore_signal(ready.at[2], inc=1, device_id={"rows": r + 1}, device_id_type=MESH)

    @pl.when(g > 0)
    def _():
        pl.semaphore_wait(ready.at[3], 1)

    @pl.when(g < G - 1)
    def _():
        pl.semaphore_signal(ready.at[3], inc=1, device_id={"gz": g + 1}, device_id_type=MESH)

    region = pl.ds(width - reach, reach)
    late[:, :, reach:] = jnp.zeros((G, rows_all, SIDE), bf16)

    @pl.when(r == 0)
    def _():
        late[:, 0:EDGE, :] = jnp.zeros((G, EDGE, reach + SIDE), bf16)

    @pl.when(r == R - 1)
    def _():
        late[:, EDGE + band :, :] = jnp.zeros((G, EDGE, reach + SIDE), bf16)

    def late_body():
        return pltpu.make_async_remote_copy(
            src_ref=cur.at[:, region], dst_ref=late.at[g, pl.ds(EDGE, band), pl.ds(0, reach)],
            send_sem=late_send.at[0], recv_sem=late_recv.at[g],
            device_id={"gz": 0}, device_id_type=MESH)

    def late_section(s, rows):
        ref = late.at[s, pl.ds(0, rows), pl.ds(0, reach)]
        return pltpu.make_async_remote_copy(
            src_ref=ref, dst_ref=ref, send_sem=late_send.at[0], recv_sem=late_recv.at[s],
            device_id={"rows": lax.rem(r + 1, R)}, device_id_type=MESH)

    def await_section(s, rows):
        @pl.when((r == 0) | (r == R - 1))
        def _():
            late_section(s, rows + EDGE).wait_recv()

        @pl.when((r > 0) & (r < R - 1))
        def _():
            late_section(s, rows + 2 * EDGE).wait_recv()

    def late_edge(up):
        source = pl.ds(0 if up else band - EDGE, EDGE)
        target = pl.ds(EDGE + band if up else 0, EDGE)
        return pltpu.make_async_remote_copy(
            src_ref=cur.at[source, region], dst_ref=late.at[g, target, pl.ds(0, reach)],
            send_sem=late_send.at[1], recv_sem=late_recv.at[g],
            device_id={"gz": 0, "rows": lax.rem(r + (R - 1 if up else 1), R)}, device_id_type=MESH)

    def late_edges(count):
        ref = late.at[0, pl.ds(0, count * EDGE), pl.ds(0, reach)]
        return pltpu.make_async_remote_copy(
            src_ref=ref, dst_ref=ref, send_sem=late_send.at[1], recv_sem=late_recv.at[0],
            device_id={"rows": lax.rem(r + 1, R)}, device_id_type=MESH)

    def late_peak():
        return pltpu.make_async_remote_copy(
            src_ref=shift_row, dst_ref=shifts.at[pl.ds(g, 1)], send_sem=late_send.at[2], recv_sem=shift_recv,
            device_id={"gz": 0}, device_id_type=MESH)

    def late_peaks():
        ref = shifts.at[pl.ds(1, G - 1)]
        return pltpu.make_async_remote_copy(
            src_ref=ref, dst_ref=ref, send_sem=late_send.at[2], recv_sem=shift_recv,
            device_id={"rows": lax.rem(r + 1, R)}, device_id_type=MESH)

    shift_row[...] = jnp.where(lane == 0, peaks[0, 0, patch_row, pgx - 1], peaks[0, 1, patch_row, pgx - 1])

    @pl.when(g == 0)
    def _():
        late[0, EDGE : EDGE + band, 0:reach] = cur[:, width - reach :]

    @pl.when(g > 0)
    def _():
        late_body().start()
        late_peak().start()

    @pl.when(r > 0)
    def _():
        late_edge(True).start()

    @pl.when(r < R - 1)
    def _():
        late_edge(False).start()

    @pl.when(g > 0)
    def _():
        edge_copy(0).wait_recv()

        @pl.when(r > 0)
        def _():
            relay_up().start()

        edge_copy(1).wait_recv()

        @pl.when(r < R - 1)
        def _():
            relay_down().start()

        @pl.when((r == 0) | (r == R - 1))
        def _():
            both_relays(1).wait_recv()

        @pl.when((r > 0) & (r < R - 1))
        def _():
            both_relays(2).wait_recv()

    @pl.when((g > 0) & (g < G - 1))
    def _():
        pl.semaphore_wait(ready.at[0], 1)

    @pl.when(g > 0)
    def _():
        pl.semaphore_signal(ready.at[0], inc=1, device_id={"gz": g - 1}, device_id_type=MESH)
        head_copy().wait_recv()

    def correlate(window, columns, gradients, down, current, keep):
        moved = jnp.dot(window, columns, preferred_element_type=f32)
        slope = jnp.dot(window, gradients, preferred_element_type=f32)
        sums = [jnp.zeros((8, 128), f32) for _ in range(5)]
        for n in range(BLOCK // 128):
            shifted[n] = moved[:, n * 128 : (n + 1) * 128]
            sloped[n] = slope[:, n * 128 : (n + 1) * 128]
        for n in range(BLOCK // 128):
            q = shifted[n, pl.ds(down, band), :]
            gy = (shifted[n, pl.ds(down + 1, band), :] - shifted[n, pl.ds(down - 1, band), :]) * 0.5
            gx = sloped[n, pl.ds(down, band), :]
            e = current(n).astype(f32) - q
            keep(n, e)
            for m, value in enumerate((gy * gy, gy * gx, gx * gx, gy * e, gx * e)):
                sums[m] = sums[m] + jnp.sum(value.reshape(band // 8, 8, 128), axis=0)
        return sums

    def body(c, z):
        @pl.when((g > 0) & (c % GROUP == 1) & (c <= grouped))
        def _():
            group_copy(c // GROUP).wait_recv()

        @pl.when((g > 0) & (c > grouped) & (c < blocks - 1))
        def _():
            middle_copy(c).wait_recv()

        @pl.when((g > 0) & (c == blocks - 1))
        def _():
            tail_copy().wait_recv()

        j = c // per_patch
        col = pl.multiple_of(c * BLOCK, BLOCK)

        def keep(n, e):
            res[0, :, pl.ds(col + n * 128, 128)] = e.astype(bf16)

        sums = correlate(prev[:, pl.ds(col, BLOCK + 2 * SIDE)], cmat[j], gmat[j], EDGE + peaks[0, 0, patch_row, j],
                         lambda n: cur[:, pl.ds(col + n * 128, 128)], keep)
        spare = acc.shape[0] // 8 - 8
        for m, value in enumerate(sums):
            place = jnp.where(c < blocks - LATE, m * pgx + j, spare + m)
            at = pl.ds(pl.multiple_of(place * 8, 8), 8)
            acc[at, :] = acc[at, :] + value
        return z

    lax.fori_loop(0, blocks - LATE, body, 0)

    @pl.when(g == 0)
    def _():
        pl.semaphore_wait(ready.at[0], 1)


    count = acc.shape[0] // 8 - 8
    totals = acc[pl.ds(0, count, stride=8), :]
    for k in range(1, 8):
        totals = totals + acc[pl.ds(k, count, stride=8), :]
    totals = jnp.sum(totals, axis=1, keepdims=True)
    place = lax.broadcasted_iota(jnp.int32, (count, 128), 0)
    for m in range(1, 5):
        place = place + jnp.where(lax.broadcasted_iota(jnp.int32, (count, 128), 0) >= m * pgx, patches - pgx, 0)
    hit = lax.broadcasted_iota(jnp.int32, (count, 128), 1) == place + patch_row * pgx
    mine = jnp.sum(jnp.where(hit, totals, 0.0), axis=0, keepdims=True)
    slot = pl.ds(r * G + g, 1)
    gather[slot, :] = mine + extra[...]

    def sum_copy(d, k):
        return pltpu.make_async_remote_copy(
            src_ref=gather.at[slot], dst_ref=gather.at[slot], send_sem=sum_send, recv_sem=sum_recv,
            device_id={"gz": g + d, "rows": lax.rem(r + k, R)}, device_id_type=MESH)

    def all_sums(count):
        return pltpu.make_async_remote_copy(
            src_ref=gather.at[pl.ds(0, count)], dst_ref=gather.at[pl.ds(0, count)],
            send_sem=sum_send, recv_sem=sum_recv, device_id={"rows": lax.rem(r + 1, R)}, device_id_type=MESH)

    def send_sums(i, z):
        d = i
        for k in range(R):
            if k:
                sum_copy(d, k).start()
            else:
                @pl.when(d > 0)
                def _():
                    sum_copy(d, k).start()
        return z

    lax.fori_loop(0, G - g, send_sums, 0)

    def late_rows(s, k):
        rows = pl.ds((R + r) * G, G)
        return pltpu.make_async_remote_copy(
            src_ref=gather.at[rows], dst_ref=gather.at[rows], send_sem=rows_send.at[s], recv_sem=rows_recv,
            device_id={"gz": s, "rows": lax.rem(r + k, R)}, device_id_type=MESH)

    def all_rows(s):
        rows = pl.ds(0, R * G)
        return pltpu.make_async_remote_copy(
            src_ref=gather.at[rows], dst_ref=gather.at[rows], send_sem=rows_send.at[s], recv_sem=rows_recv,
            device_id={"rows": lax.rem(r + 1, R)}, device_id_type=MESH)

    @pl.when(g == 0)
    def _():
        late_peaks().wait_recv()
        await_section(G - 1, band)

        def assist(i, z):
            s = G - i

            @pl.when(i < G - 1)
            def _():
                await_section(s - 1, band)

            @pl.when(i == G - 1)
            def _():
                await_section(0, 0)

            a = shifts[s, 0]
            b = shifts[s, 1]
            cmat[0] = jnp.where(cdiff == b, 1.0, 0.0).astype(bf16)
            gmat[0] = jnp.where(cdiff == b + 1, 0.5, jnp.where(cdiff == b - 1, -0.5, 0.0)).astype(bf16)
            both = [jnp.zeros((8, 128), f32) for _ in range(5)]
            for k in range(LATE):
                found = correlate(
                    late[s - 1, :, k * BLOCK : k * BLOCK + BLOCK + 2 * SIDE], cmat[0], gmat[0], EDGE + a,
                    lambda n: late[s, EDGE : EDGE + band, SIDE + k * BLOCK + n * 128 : SIDE + k * BLOCK + n * 128 + 128],
                    lambda n, e: None)
                both = [old + new for old, new in zip(both, found)]
            for m, value in enumerate(both):
                late_acc[pl.ds(pl.multiple_of((m * G + s) * 8, 8), 8), :] = value
            return z

        late_acc[...] = jnp.zeros_like(late_acc)
        lax.fori_loop(1, G, assist, 0)

        sums = late_acc[pl.ds(0, 5 * G, stride=8), :]
        for k in range(1, 8):
            sums = sums + late_acc[pl.ds(k, 5 * G, stride=8), :]
        sums = jnp.sum(sums, axis=1, keepdims=True)
        wide = lax.broadcasted_iota(jnp.int32, (G, 128), 1)
        lines = jnp.zeros((G, 128), f32)
        for m in range(5):
            lines = jnp.where(wide == m * patches + patch_row * pgx + pgx - 1, sums[m * G : (m + 1) * G], lines)
        gather[pl.ds((R + r) * G, G), :] = lines

        def hand_out(s, z):
            for k in range(R):
                late_rows(s, k).start()
            return z

        lax.fori_loop(1, G, hand_out, 0)

    lax.fori_loop(blocks - LATE, blocks, body, 0)

    @pl.when(g < G - 1)
    def _():
        pltpu.make_async_remote_copy(
            src_ref=cur, dst_ref=cur, send_sem=send_sem, recv_sem=recv_sem.at[0],
            device_id={"gz": ahead}, device_id_type=MESH).wait_send()

    @pl.when((g > 0) & ((r == 0) | (r == R - 1)))
    def _():
        both_relays(1).wait_send()

    @pl.when((g > 0) & (r > 0) & (r < R - 1))
    def _():
        both_relays(2).wait_send()

    @pl.when(g > 0)
    def _():
        late_body().wait_send()
        late_peak().wait_send()

    @pl.when((r == 0) | (r == R - 1))
    def _():
        late_edges(1).wait_send()

    @pl.when((r > 0) & (r < R - 1))
    def _():
        late_edges(2).wait_send()

    @pl.when(g == 0)
    def _():
        lax.fori_loop(1, G, lambda s, z: (all_rows(s).wait_send(), z)[1], 0)

    @pl.when(g > 0)
    def _():
        all_rows(0).wait_recv()

    for s in range(G):
        @pl.when(g == s)
        def _():
            all_sums(R * (G - s) - 1).wait_send()
            all_sums(R * (s + 1) - 1).wait_recv()

    full = gather[0:G]
    for k in range(1, 2 * R):
        full = full + gather[k * G : (k + 1) * G]

    def moment(m):
        return pltpu.roll(full, 128 - m * patches, 1)

    damping = LAMBDA * PATCH * PATCH
    first = full + damping
    cross = moment(1)
    second = moment(2) + damping
    pull_y = moment(3)
    pull_x = moment(4)
    det = first * second - cross * cross
    valid = lax.broadcasted_iota(jnp.int32, (G, 128), 1) < patches
    off_y = jnp.where(valid, moment(5) + (second * pull_y - cross * pull_x) / det, 0.0)
    off_x = jnp.where(valid, moment(6) + (first * pull_x - cross * pull_y) / det, 0.0)
    ty = jnp.zeros((1, 128), f32)
    tx = jnp.zeros((1, 128), f32)
    for p in range(patches):
        ty = jnp.where(lane == p, float(table[0, p]), ty)
        tx = jnp.where(lane == p, float(table[1, p]), tx)

    def lanes(value):
        return jnp.broadcast_to(jnp.sum(value, axis=1, keepdims=True), (G, 128))

    yy = 1.0 + lanes(off_y * ty) / height
    yx = lanes(off_y * tx) / width
    xy = lanes(off_x * ty) / height
    xx = 1.0 + lanes(off_x * tx) / width
    uy = jnp.zeros((1, 128), f32)
    ux = jnp.zeros((1, 128), f32)
    for s in range(G):
        at = slice(s, s + 1)
        step_y = yy[at] * uy + yx[at] * ux + off_y[at]
        step_x = xy[at] * uy + xx[at] * ux + off_x[at]
        uy = jnp.where(s <= g, step_y, uy)
        ux = jnp.where(s <= g, step_x, ux)
    chosen = lax.broadcasted_iota(jnp.int32, (G, 128), 0) == g
    nodes[0:1] = uy
    nodes[1:2] = ux
    nodes[2:3] = jnp.sum(jnp.where(chosen, off_y, 0.0), axis=0, keepdims=True)
    nodes[3:4] = jnp.sum(jnp.where(chosen, off_x, 0.0), axis=0, keepdims=True)
    nodes[4:8] = jnp.zeros((4, 128), f32)


def spread_out(pgy, pgx, nodes, res_in, field, offsets, res_out, buf, out_sem, field_sem):
    band, width = field.shape[2], field.shape[3]
    f32 = jnp.float32
    put = pltpu.make_async_copy(res_in, res_out, out_sem)
    put.start()
    cols = (lax.broadcasted_iota(jnp.int32, (8, width), 1).astype(f32) + 0.5) / PATCH - 0.5
    cols = jnp.clip(cols, 0.0, pgx - 1.0)
    weights = [jnp.maximum(0.0, 1.0 - jnp.abs(cols - j)) for j in range(pgx)]
    part = 32
    for k in range(2):
        wide = []
        for i in range(pgy):
            line = jnp.zeros((8, width), f32)
            for j in range(pgx):
                p = i * pgx + j
                line = line + weights[j] * nodes[k : k + 1, p : p + 1]
            wide.append(line)
        for t in range(band // part):
            slot = 0 if pgy == 1 else t
            for q in range(0, part, 8) if pgy > 1 or t == 0 else ():
                if pgy == 1:
                    block = wide[0]
                else:
                    rows = (lax.broadcasted_iota(jnp.int32, (8, 1), 0) + lax.axis_index("rows") * band).astype(f32)
                    pos = jnp.clip((rows + (t * part + q + 0.5)) / PATCH - 0.5, 0.0, pgy - 1.0)
                    block = sum(jnp.maximum(0.0, 1.0 - jnp.abs(pos - i)) * wide[i] for i in range(pgy))
                buf[k, slot * part + q : slot * part + q + 8, :] = block
            pltpu.make_async_copy(
                buf.at[k, pl.ds(slot * part, part), :], field.at[0, k, pl.ds(t * part, part), :], field_sem).start()
    offsets[...] = nodes[2:4, 0 : pgy * pgx]
    put.wait()
    pltpu.make_async_copy(field, field, field_sem).wait()


def per_device(G, R, sections, peaks):
    band, width = sections.shape[1:]
    height = band * R
    pgy, pgx = height // PATCH, width // PATCH
    blocks = width // BLOCK
    f32, bf16 = jnp.float32, jnp.bfloat16
    table = fit_table(pgy, pgx, PATCH, height, width).astype(np.float32)
    vmem = pl.BlockSpec(memory_space=pltpu.VMEM)
    anywhere = pl.BlockSpec(memory_space=pl.ANY)
    dma = pltpu.SemaphoreType.DMA
    padded = -(-5 * pgx // 8) * 8
    grouped = (blocks - 4) // GROUP * GROUP
    arrivals = 2 + blocks - grouped + grouped // GROUP
    residual, nodes = pl.pallas_call(
        functools.partial(register, G, R, pgy, pgx, table),
        name="register",
        out_shape=(jax.ShapeDtypeStruct((1, band, width), bf16), jax.ShapeDtypeStruct((8, 128), f32)),
        in_specs=[anywhere, anywhere],
        out_specs=(vmem, vmem),
        scratch_shapes=[
            pltpu.VMEM((band + 2 * EDGE, width + 2 * SIDE), bf16),
            pltpu.VMEM((band, width), bf16),
            pltpu.VMEM((pgx, BLOCK + 2 * SIDE, BLOCK), bf16),
            pltpu.VMEM((pgx, BLOCK + 2 * SIDE, BLOCK), bf16),
            pltpu.VMEM((BLOCK // 128, band + 2 * EDGE, 128), f32),
            pltpu.VMEM((BLOCK // 128, band + 2 * EDGE, 128), f32),
            pltpu.VMEM((8 * (padded + 8), 128), f32),
            pltpu.VMEM((2 * R * G, 128), f32),
            pltpu.VMEM((1, 128), f32),
            pltpu.SMEM((1, 2, pgy, pgx), jnp.int32),
            dma, dma((3,)), pltpu.SemaphoreType.REGULAR((4,)), dma, dma((arrivals,)), dma, dma,
            dma, dma,
            pltpu.VMEM((G, band + 2 * EDGE, LATE * BLOCK + 2 * SIDE), bf16),
            pltpu.VMEM((1, 128), jnp.int32), pltpu.VMEM((G, 128), jnp.int32),
            dma((3,)), dma((G,)), dma, dma((G,)), dma,
            pltpu.VMEM((5 * G * 8, 128), f32),
        ],
        compiler_params=pltpu.CompilerParams(collective_id=0, has_side_effects=True, vmem_limit_bytes=40 * 2**20),
    )(pltpu.with_memory_space_constraint(peaks, pltpu.HBM), pltpu.with_memory_space_constraint(sections, pltpu.HBM))
    field, offsets, residual = pl.pallas_call(
        functools.partial(spread_out, pgy, pgx),
        name="spread_out",
        out_shape=(
            jax.ShapeDtypeStruct((1, 2, band, width), f32),
            jax.ShapeDtypeStruct((2, pgy * pgx), f32),
            jax.ShapeDtypeStruct((1, band, width), bf16),
        ),
        in_specs=[vmem, vmem],
        out_specs=(anywhere, vmem, anywhere),
        scratch_shapes=[pltpu.VMEM((2, 32 if pgy == 1 else band, width), f32), dma, dma],
        compiler_params=pltpu.CompilerParams(vmem_limit_bytes=20 * 2**20),
    )(nodes, residual)
    return field, offsets.reshape(1, 2, pgy, pgx), residual


def solution(mesh):
    return jax.shard_map(
        functools.partial(per_device, mesh.shape["gz"], mesh.shape["rows"]),
        mesh=mesh,
        in_specs=(P("gz", "rows", None), P("gz", None, None, None)),
        out_specs=(P("gz", None, "rows", None), P("gz", None, None, None), P("gz", "rows", None)),
        check_vma=False,
    )
```

```python
import functools

import jax
import jax.numpy as jnp
import numpy as np
from jax import lax
from jax.experimental import pallas as pl
from jax.experimental.pallas import tpu as pltpu
from jax.sharding import PartitionSpec as P

PATCH = 1024
MAXOFF = 16
LAMBDA = 0.002
RIDGE = 0.05
EDGE = 32
SIDE = 128
BLOCK = 256
GROUP = 4
LATE = 2
MESH = pl.DeviceIdType.MESH


def invert_three(matrix):
    a, b, c = (matrix[0, 0], matrix[0, 1], matrix[0, 2])
    d, e, f = (matrix[1, 0], matrix[1, 1], matrix[1, 2])
    g, h, k = (matrix[2, 0], matrix[2, 1], matrix[2, 2])
    cof = np.array(
        [
            [e * k - f * h, c * h - b * k, b * f - c * e],
            [f * g - d * k, a * k - c * g, c * d - a * f],
            [d * h - e * g, b * g - a * h, a * e - b * d],
        ]
    )
    return cof / (a * (e * k - f * h) - b * (d * k - f * g) + c * (d * h - e * g))


def fit_table(pgy, pgx, patch, height, width):
    yy = ((np.arange(pgy) + 0.5) * patch - height / 2.0) / height
    xx = ((np.arange(pgx) + 0.5) * patch - width / 2.0) / width
    design = np.stack([np.repeat(yy, pgx), np.tile(xx, pgy), np.ones(pgy * pgx)], 1)
    ridge_matrix = np.array([[RIDGE, 0.0, 0.0], [0.0, RIDGE, 0.0], [0.0, 0.0, 0.0]])
    gram = design.T @ design + ridge_matrix
    return invert_three(gram) @ design.T


def register(G, R, pgy, pgx, table, peaks_hbm, sec, res, nodes, prev, cur, cmat, gmat, shifted, sloped, acc,
             gather, extra, peaks, peak_sem, cur_sem, ready, send_sem, recv_sem, rel_send, rel_recv,
             sum_send, sum_recv, late, shift_row, shifts, late_send, late_recv, shift_recv, rows_send, rows_recv, late_acc):
    band, width = sec.shape[1], sec.shape[2]
    height = band * R
    blocks = width // BLOCK
    per_patch = PATCH // BLOCK
    patches = pgy * pgx
    g, r = lax.axis_index("gz"), lax.axis_index("rows")
    f32, bf16 = jnp.float32, jnp.bfloat16

    spans = ((0, EDGE), (band - EDGE, EDGE), (EDGE, band - 2 * EDGE))

    def load(k):
        rows = pl.ds(*spans[k])
        return pltpu.make_async_copy(sec.at[0, rows, :], cur.at[rows, :], cur_sem.at[k])

    gather[...] = jnp.zeros_like(gather)
    barrier = pltpu.get_barrier_semaphore()

    @pl.when(g > 0)
    def _():
        pl.semaphore_signal(barrier, inc=1, device_id={"gz": g - 1}, device_id_type=MESH)

    for k in range(3):
        load(k).start()
    peak_load = pltpu.make_async_copy(peaks_hbm, peaks, peak_sem)
    peak_load.start()

    @pl.when(r < R - 1)
    def _():
        pl.semaphore_signal(barrier, inc=1, device_id={"rows": r + 1}, device_id_type=MESH)

    @pl.when(g < G - 1)
    def _():
        pl.semaphore_signal(barrier, inc=1, device_id={"gz": g + 1}, device_id_type=MESH)

    greets = [jnp.where(near, 1, 0) for near in (g > 0, g < G - 1, r > 0)]
    pl.semaphore_wait(barrier, sum(greets))
    rows_all = band + 2 * EDGE
    reach = LATE * BLOCK + SIDE
    ahead = lax.rem(g + 1, G)

    def edge_copy(which):
        row = 0 if which == 0 else band - EDGE
        return pltpu.make_async_remote_copy(
            src_ref=cur.at[pl.ds(row, EDGE), :],
            dst_ref=prev.at[pl.ds(EDGE + row, EDGE), pl.ds(SIDE, width)],
            send_sem=send_sem, recv_sem=recv_sem.at[which],
            device_id={"gz": ahead}, device_id_type=MESH)

    def span_copy(index, col, count):
        return pltpu.make_async_remote_copy(
            src_ref=cur.at[pl.ds(EDGE, band - 2 * EDGE), pl.ds(col, count)],
            dst_ref=prev.at[pl.ds(2 * EDGE, band - 2 * EDGE), pl.ds(SIDE + col, count)],
            send_sem=send_sem, recv_sem=recv_sem.at[2 + index],
            device_id={"gz": ahead}, device_id_type=MESH)

    def head_copy():
        return span_copy(0, 0, BLOCK + SIDE)

    grouped = (blocks - 4) // GROUP * GROUP
    singles = grouped // GROUP - grouped

    def group_copy(n):
        k = n * GROUP + 1
        return span_copy(1 + n, pl.multiple_of(k * BLOCK + SIDE, SIDE), GROUP * BLOCK)

    def middle_copy(k):
        return span_copy(singles + k, pl.multiple_of(k * BLOCK + SIDE, SIDE), BLOCK)

    def tail_copy():
        return span_copy(singles + blocks - 1, width - BLOCK + SIDE, BLOCK - SIDE)

    def relay_up():
        return pltpu.make_async_remote_copy(
            src_ref=prev.at[pl.ds(EDGE, EDGE), pl.ds(SIDE, width)],
            dst_ref=prev.at[pl.ds(EDGE + band, EDGE), pl.ds(SIDE, width)],
            send_sem=rel_send, recv_sem=rel_recv,
            device_id={"rows": lax.rem(r + R - 1, R)}, device_id_type=MESH)

    def relay_down():
        return pltpu.make_async_remote_copy(
            src_ref=prev.at[pl.ds(band, EDGE), pl.ds(SIDE, width)],
            dst_ref=prev.at[pl.ds(0, EDGE), pl.ds(SIDE, width)],
            send_sem=rel_send, recv_sem=rel_recv,
            device_id={"rows": lax.rem(r + 1, R)}, device_id_type=MESH)

    def both_relays(count):
        rows = pl.ds(0, count * EDGE)
        return pltpu.make_async_remote_copy(
            src_ref=cur.at[rows, :], dst_ref=cur.at[rows, :], send_sem=rel_send, recv_sem=rel_recv,
            device_id={"rows": lax.rem(r + 1, R)}, device_id_type=MESH)

    for which in (0, 1):
        load(which).wait()

        @pl.when(g < G - 1)
        def _():
            edge_copy(which).start()

    load(2).wait()

    @pl.when(g < G - 1)
    def _():
        head_copy().start()
        lax.fori_loop(0, grouped // GROUP, lambda n, z: (group_copy(n).start(), z)[1], 0)
        lax.fori_loop(grouped + 1, blocks - 1, lambda k, z: (middle_copy(k).start(), z)[1], 0)
        tail_copy().start()

    prev[:, 0:SIDE] = jnp.zeros((rows_all, SIDE), bf16)
    prev[:, SIDE + width :] = jnp.zeros((rows_all, SIDE), bf16)

    @pl.when(r == 0)
    def _():
        prev[0:EDGE, :] = jnp.zeros((EDGE, width + 2 * SIDE), bf16)

    @pl.when(r == R - 1)
    def _():
        prev[EDGE + band :, :] = jnp.zeros((EDGE, width + 2 * SIDE), bf16)

    @pl.when(g == 0)
    def _():
        def clear(t, z):
            prev[pl.ds(pl.multiple_of(t * EDGE, EDGE), EDGE), :] = jnp.zeros((EDGE, width + 2 * SIDE), bf16)
            return z

        lax.fori_loop(0, rows_all // EDGE, clear, 0)

    patch_row = r * band // PATCH
    peak_load.wait()
    ck = lax.broadcasted_iota(jnp.int32, (BLOCK + 2 * SIDE, BLOCK), 0)
    cn = lax.broadcasted_iota(jnp.int32, (BLOCK + 2 * SIDE, BLOCK), 1)
    cdiff = ck - cn - SIDE

    acc[...] = jnp.zeros_like(acc)

    lane = lax.broadcasted_iota(jnp.int32, (1, 128), 1)
    own_peaks = jnp.zeros((1, 128), f32)
    for i in range(pgy):
        for j in range(pgx):
            p = i * pgx + j
            own_peaks = jnp.where(lane == 5 * patches + p, peaks[0, 0, i, j].astype(f32), own_peaks)
            own_peaks = jnp.where(lane == 6 * patches + p, peaks[0, 1, i, j].astype(f32), own_peaks)
    extra[...] = jnp.where(r == 0, own_peaks, jnp.zeros((1, 128), f32))

    @pl.when(r < R - 1)
    def _():
        pl.semaphore_wait(ready.at[1], 1)

    @pl.when(r > 0)
    def _():
        pl.semaphore_signal(ready.at[1], inc=1, device_id={"rows": r - 1}, device_id_type=MESH)
        pl.semaphore_wait(ready.at[2], 1)

    @pl.when(r < R - 1)
    def _():
        pl.semaphore_signal(ready.at[2], inc=1, device_id={"rows": r + 1}, device_id_type=MESH)

    @pl.when(g > 0)
    def _():
        pl.semaphore_wait(ready.at[3], 1)

    @pl.when(g < G - 1)
    def _():
        pl.semaphore_signal(ready.at[3], inc=1, device_id={"gz": g + 1}, device_id_type=MESH)

    region = pl.ds(width - reach, reach)
    late[:, :, reach:] = jnp.zeros((G, rows_all, SIDE), bf16)

    @pl.when(r == 0)
    def _():
        late[:, 0:EDGE, :] = jnp.zeros((G, EDGE, reach + SIDE), bf16)

    @pl.when(r == R - 1)
    def _():
        late[:, EDGE + band :, :] = jnp.zeros((G, EDGE, reach + SIDE), bf16)

    def late_body():
        return pltpu.make_async_remote_copy(
            src_ref=cur.at[:, region], dst_ref=late.at[g, pl.ds(EDGE, band), pl.ds(0, reach)],
            send_sem=late_send.at[0], recv_sem=late_recv.at[g],
            device_id={"gz": 0}, device_id_type=MESH)

    def late_section(s, rows):
        ref = late.at[s, pl.ds(0, rows), pl.ds(0, reach)]
        return pltpu.make_async_remote_copy(
            src_ref=ref, dst_ref=ref, send_sem=late_send.at[0], recv_sem=late_recv.at[s],
            device_id={"rows": lax.rem(r + 1, R)}, device_id_type=MESH)

    def await_section(s, rows):
        @pl.when((r == 0) | (r == R - 1))
        def _():
            late_section(s, rows + EDGE).wait_recv()

        @pl.when((r > 0) & (r < R - 1))
        def _():
            late_section(s, rows + 2 * EDGE).wait_recv()

    def late_edge(up):
        source = pl.ds(0 if up else band - EDGE, EDGE)
        target = pl.ds(EDGE + band if up else 0, EDGE)
        return pltpu.make_async_remote_copy(
            src_ref=cur.at[source, region], dst_ref=late.at[g, target, pl.ds(0, reach)],
            send_sem=late_send.at[1], recv_sem=late_recv.at[g],
            device_id={"gz": 0, "rows": lax.rem(r + (R - 1 if up else 1), R)}, device_id_type=MESH)

    def late_edges(count):
        ref = late.at[0, pl.ds(0, count * EDGE), pl.ds(0, reach)]
        return pltpu.make_async_remote_copy(
            src_ref=ref, dst_ref=ref, send_sem=late_send.at[1], recv_sem=late_recv.at[0],
            device_id={"rows": lax.rem(r + 1, R)}, device_id_type=MESH)

    def late_peak():
        return pltpu.make_async_remote_copy(
            src_ref=shift_row, dst_ref=shifts.at[pl.ds(g, 1)], send_sem=late_send.at[2], recv_sem=shift_recv,
            device_id={"gz": 0}, device_id_type=MESH)

    def late_peaks():
        ref = shifts.at[pl.ds(1, G - 1)]
        return pltpu.make_async_remote_copy(
            src_ref=ref, dst_ref=ref, send_sem=late_send.at[2], recv_sem=shift_recv,
            device_id={"rows": lax.rem(r + 1, R)}, device_id_type=MESH)

    shift_row[...] = jnp.where(lane == 0, peaks[0, 0, patch_row, pgx - 1], peaks[0, 1, patch_row, pgx - 1])

    @pl.when(g == 0)
    def _():
        late[0, EDGE : EDGE + band, 0:reach] = cur[:, width - reach :]

    @pl.when(g > 0)
    def _():
        late_body().start()
        late_peak().start()

    @pl.when(r > 0)
    def _():
        late_edge(True).start()

    @pl.when(r < R - 1)
    def _():
        late_edge(False).start()

    @pl.when(g > 0)
    def _():
        edge_copy(0).wait_recv()

        @pl.when(r > 0)
        def _():
            relay_up().start()

        edge_copy(1).wait_recv()

        @pl.when(r < R - 1)
        def _():
            relay_down().start()

        @pl.when((r == 0) | (r == R - 1))
        def _():
            both_relays(1).wait_recv()

        @pl.when((r > 0) & (r < R - 1))
        def _():
            both_relays(2).wait_recv()

    @pl.when((g > 0) & (g < G - 1))
    def _():
        pl.semaphore_wait(ready.at[0], 1)

    @pl.when(g > 0)
    def _():
        pl.semaphore_signal(ready.at[0], inc=1, device_id={"gz": g - 1}, device_id_type=MESH)
        head_copy().wait_recv()

    def correlate(window, columns, gradients, down, current, keep):
        moved = jnp.dot(window, columns, preferred_element_type=f32)
        slope = jnp.dot(window, gradients, preferred_element_type=f32)
        sums = [jnp.zeros((8, 128), f32) for _ in range(5)]
        for n in range(BLOCK // 128):
            shifted[n] = moved[:, n * 128 : (n + 1) * 128]
            sloped[n] = slope[:, n * 128 : (n + 1) * 128]
        for n in range(BLOCK // 128):
            q = shifted[n, pl.ds(down, band), :]
            gy = (shifted[n, pl.ds(down + 1, band), :] - shifted[n, pl.ds(down - 1, band), :]) * 0.5
            gx = sloped[n, pl.ds(down, band), :]
            e = current(n).astype(f32) - q
            keep(n, e)
            for m, value in enumerate((gy * gy, gy * gx, gx * gx, gy * e, gx * e)):
                sums[m] = sums[m] + jnp.sum(value.reshape(band // 8, 8, 128), axis=0)
        return sums

    def body(c, z):
        @pl.when((g > 0) & (c % GROUP == 1) & (c <= grouped))
        def _():
            group_copy(c // GROUP).wait_recv()

        @pl.when((g > 0) & (c > grouped) & (c < blocks - 1))
        def _():
            middle_copy(c).wait_recv()

        @pl.when((g > 0) & (c == blocks - 1))
        def _():
            tail_copy().wait_recv()

        j = c // per_patch
        col = pl.multiple_of(c * BLOCK, BLOCK)

        def keep(n, e):
            res[0, :, pl.ds(col + n * 128, 128)] = e.astype(bf16)

        b = peaks[0, 1, patch_row, j]
        cmat[0] = jnp.where(cdiff == b, 1.0, 0.0).astype(bf16)
        gmat[0] = jnp.where(cdiff == b + 1, 0.5, jnp.where(cdiff == b - 1, -0.5, 0.0)).astype(bf16)
        sums = correlate(prev[:, pl.ds(col, BLOCK + 2 * SIDE)], cmat[0], gmat[0], EDGE + peaks[0, 0, patch_row, j],
                         lambda n: cur[:, pl.ds(col + n * 128, 128)], keep)
        spare = acc.shape[0] // 8 - 8
        for m, value in enumerate(sums):
            place = jnp.where(c < blocks - LATE, m * pgx + j, spare + m)
            at = pl.ds(pl.multiple_of(place * 8, 8), 8)
            acc[at, :] = acc[at, :] + value
        return z

    lax.fori_loop(0, blocks - LATE, body, 0)

    @pl.when(g == 0)
    def _():
        pl.semaphore_wait(ready.at[0], 1)


    count = acc.shape[0] // 8 - 8
    totals = acc[pl.ds(0, count, stride=8), :]
    for k in range(1, 8):
        totals = totals + acc[pl.ds(k, count, stride=8), :]
    totals = jnp.sum(totals, axis=1, keepdims=True)
    place = lax.broadcasted_iota(jnp.int32, (count, 128), 0)
    for m in range(1, 5):
        place = place + jnp.where(lax.broadcasted_iota(jnp.int32, (count, 128), 0) >= m * pgx, patches - pgx, 0)
    hit = lax.broadcasted_iota(jnp.int32, (count, 128), 1) == place + patch_row * pgx
    mine = jnp.sum(jnp.where(hit, totals, 0.0), axis=0, keepdims=True)
    slot = pl.ds(r * G + g, 1)
    gather[slot, :] = mine + extra[...]

    def sum_copy(d, k):
        return pltpu.make_async_remote_copy(
            src_ref=gather.at[slot], dst_ref=gather.at[slot], send_sem=sum_send, recv_sem=sum_recv,
            device_id={"gz": g + d, "rows": lax.rem(r + k, R)}, device_id_type=MESH)

    def all_sums(count):
        return pltpu.make_async_remote_copy(
            src_ref=gather.at[pl.ds(0, count)], dst_ref=gather.at[pl.ds(0, count)],
            send_sem=sum_send, recv_sem=sum_recv, device_id={"rows": lax.rem(r + 1, R)}, device_id_type=MESH)

    def send_sums(i, z):
        d = i
        for k in range(R):
            if k:
                sum_copy(d, k).start()
            else:
                @pl.when(d > 0)
                def _():
                    sum_copy(d, k).start()
        return z

    lax.fori_loop(0, G - g, send_sums, 0)

    def late_rows(s, k):
        rows = pl.ds((R + r) * G, G)
        return pltpu.make_async_remote_copy(
            src_ref=gather.at[rows], dst_ref=gather.at[rows], send_sem=rows_send.at[s], recv_sem=rows_recv,
            device_id={"gz": s, "rows": lax.rem(r + k, R)}, device_id_type=MESH)

    def all_rows(s):
        rows = pl.ds(0, R * G)
        return pltpu.make_async_remote_copy(
            src_ref=gather.at[rows], dst_ref=gather.at[rows], send_sem=rows_send.at[s], recv_sem=rows_recv,
            device_id={"rows": lax.rem(r + 1, R)}, device_id_type=MESH)

    @pl.when(g == 0)
    def _():
        late_peaks().wait_recv()
        await_section(G - 1, band)

        def assist(i, z):
            s = G - i

            @pl.when(i < G - 1)
            def _():
                await_section(s - 1, band)

            @pl.when(i == G - 1)
            def _():
                await_section(0, 0)

            a = shifts[s, 0]
            b = shifts[s, 1]
            cmat[0] = jnp.where(cdiff == b, 1.0, 0.0).astype(bf16)
            gmat[0] = jnp.where(cdiff == b + 1, 0.5, jnp.where(cdiff == b - 1, -0.5, 0.0)).astype(bf16)
            both = [jnp.zeros((8, 128), f32) for _ in range(5)]
            for k in range(LATE):
                found = correlate(
                    late[s - 1, :, k * BLOCK : k * BLOCK + BLOCK + 2 * SIDE], cmat[0], gmat[0], EDGE + a,
                    lambda n: late[s, EDGE : EDGE + band, SIDE + k * BLOCK + n * 128 : SIDE + k * BLOCK + n * 128 + 128],
                    lambda n, e: None)
                both = [old + new for old, new in zip(both, found)]
            for m, value in enumerate(both):
                late_acc[pl.ds(pl.multiple_of((m * G + s) * 8, 8), 8), :] = value
            return z

        late_acc[...] = jnp.zeros_like(late_acc)
        lax.fori_loop(1, G, assist, 0)

        sums = late_acc[pl.ds(0, 5 * G, stride=8), :]
        for k in range(1, 8):
            sums = sums + late_acc[pl.ds(k, 5 * G, stride=8), :]
        sums = jnp.sum(sums, axis=1, keepdims=True)
        wide = lax.broadcasted_iota(jnp.int32, (G, 128), 1)
        lines = jnp.zeros((G, 128), f32)
        for m in range(5):
            lines = jnp.where(wide == m * patches + patch_row * pgx + pgx - 1, sums[m * G : (m + 1) * G], lines)
        gather[pl.ds((R + r) * G, G), :] = lines

        def hand_out(s, z):
            for k in range(R):
                late_rows(s, k).start()
            return z

        lax.fori_loop(1, G, hand_out, 0)

    lax.fori_loop(blocks - LATE, blocks, body, 0)

    @pl.when(g < G - 1)
    def _():
        pltpu.make_async_remote_copy(
            src_ref=cur, dst_ref=cur, send_sem=send_sem, recv_sem=recv_sem.at[0],
            device_id={"gz": ahead}, device_id_type=MESH).wait_send()

    @pl.when((g > 0) & ((r == 0) | (r == R - 1)))
    def _():
        both_relays(1).wait_send()

    @pl.when((g > 0) & (r > 0) & (r < R - 1))
    def _():
        both_relays(2).wait_send()

    @pl.when(g > 0)
    def _():
        late_body().wait_send()
        late_peak().wait_send()

    @pl.when((r == 0) | (r == R - 1))
    def _():
        late_edges(1).wait_send()

    @pl.when((r > 0) & (r < R - 1))
    def _():
        late_edges(2).wait_send()

    @pl.when(g == 0)
    def _():
        lax.fori_loop(1, G, lambda s, z: (all_rows(s).wait_send(), z)[1], 0)

    @pl.when(g > 0)
    def _():
        all_rows(0).wait_recv()

    for s in range(G):
        @pl.when(g == s)
        def _():
            all_sums(R * (G - s) - 1).wait_send()
            all_sums(R * (s + 1) - 1).wait_recv()

    full = gather[0:G]
    for k in range(1, 2 * R):
        full = full + gather[k * G : (k + 1) * G]

    def moment(m):
        return pltpu.roll(full, 128 - m * patches, 1)

    damping = LAMBDA * PATCH * PATCH
    first = full + damping
    cross = moment(1)
    second = moment(2) + damping
    pull_y = moment(3)
    pull_x = moment(4)
    det = first * second - cross * cross
    valid = lax.broadcasted_iota(jnp.int32, (G, 128), 1) < patches
    off_y = jnp.where(valid, moment(5) + (second * pull_y - cross * pull_x) / det, 0.0)
    off_x = jnp.where(valid, moment(6) + (first * pull_x - cross * pull_y) / det, 0.0)
    ty = jnp.zeros((1, 128), f32)
    tx = jnp.zeros((1, 128), f32)
    for p in range(patches):
        ty = jnp.where(lane == p, float(table[0, p]), ty)
        tx = jnp.where(lane == p, float(table[1, p]), tx)

    def lanes(value):
        return jnp.broadcast_to(jnp.sum(value, axis=1, keepdims=True), (G, 128))

    yy = 1.0 + lanes(off_y * ty) / height
    yx = lanes(off_y * tx) / width
    xy = lanes(off_x * ty) / height
    xx = 1.0 + lanes(off_x * tx) / width
    uy = jnp.zeros((1, 128), f32)
    ux = jnp.zeros((1, 128), f32)
    for s in range(G):
        at = slice(s, s + 1)
        step_y = yy[at] * uy + yx[at] * ux + off_y[at]
        step_x = xy[at] * uy + xx[at] * ux + off_x[at]
        uy = jnp.where(s <= g, step_y, uy)
        ux = jnp.where(s <= g, step_x, ux)
    chosen = lax.broadcasted_iota(jnp.int32, (G, 128), 0) == g
    nodes[0:1] = uy
    nodes[1:2] = ux
    nodes[2:3] = jnp.sum(jnp.where(chosen, off_y, 0.0), axis=0, keepdims=True)
    nodes[3:4] = jnp.sum(jnp.where(chosen, off_x, 0.0), axis=0, keepdims=True)
    nodes[4:8] = jnp.zeros((4, 128), f32)


def spread_out(pgy, pgx, nodes, res_in, field, offsets, res_out, buf, out_sem, field_sem):
    band, width = field.shape[2], field.shape[3]
    f32 = jnp.float32
    put = pltpu.make_async_copy(res_in, res_out, out_sem)
    put.start()
    cols = (lax.broadcasted_iota(jnp.int32, (8, width), 1).astype(f32) + 0.5) / PATCH - 0.5
    cols = jnp.clip(cols, 0.0, pgx - 1.0)
    weights = [jnp.maximum(0.0, 1.0 - jnp.abs(cols - j)) for j in range(pgx)]
    part = 32
    for k in range(2):
        wide = []
        for i in range(pgy):
            line = jnp.zeros((8, width), f32)
            for j in range(pgx):
                p = i * pgx + j
                line = line + weights[j] * nodes[k : k + 1, p : p + 1]
            wide.append(line)
        for t in range(band // part):
            slot = 0 if pgy == 1 else t
            for q in range(0, part, 8) if pgy > 1 or t == 0 else ():
                if pgy == 1:
                    block = wide[0]
                else:
                    rows = (lax.broadcasted_iota(jnp.int32, (8, 1), 0) + lax.axis_index("rows") * band).astype(f32)
                    pos = jnp.clip((rows + (t * part + q + 0.5)) / PATCH - 0.5, 0.0, pgy - 1.0)
                    block = sum(jnp.maximum(0.0, 1.0 - jnp.abs(pos - i)) * wide[i] for i in range(pgy))
                buf[k, slot * part + q : slot * part + q + 8, :] = block
            pltpu.make_async_copy(
                buf.at[k, pl.ds(slot * part, part), :], field.at[0, k, pl.ds(t * part, part), :], field_sem).start()
    offsets[...] = nodes[2:4, 0 : pgy * pgx]
    put.wait()
    pltpu.make_async_copy(field, field, field_sem).wait()


def per_device(G, R, sections, peaks):
    band, width = sections.shape[1:]
    height = band * R
    pgy, pgx = height // PATCH, width // PATCH
    blocks = width // BLOCK
    f32, bf16 = jnp.float32, jnp.bfloat16
    table = fit_table(pgy, pgx, PATCH, height, width).astype(np.float32)
    vmem = pl.BlockSpec(memory_space=pltpu.VMEM)
    anywhere = pl.BlockSpec(memory_space=pl.ANY)
    dma = pltpu.SemaphoreType.DMA
    padded = -(-5 * pgx // 8) * 8
    grouped = (blocks - 4) // GROUP * GROUP
    arrivals = 2 + blocks - grouped + grouped // GROUP
    residual, nodes = pl.pallas_call(
        functools.partial(register, G, R, pgy, pgx, table),
        name="register",
        out_shape=(jax.ShapeDtypeStruct((1, band, width), bf16), jax.ShapeDtypeStruct((8, 128), f32)),
        in_specs=[anywhere, anywhere],
        out_specs=(vmem, vmem),
        scratch_shapes=[
            pltpu.VMEM((band + 2 * EDGE, width + 2 * SIDE), bf16),
            pltpu.VMEM((band, width), bf16),
            pltpu.VMEM((1, BLOCK + 2 * SIDE, BLOCK), bf16),
            pltpu.VMEM((1, BLOCK + 2 * SIDE, BLOCK), bf16),
            pltpu.VMEM((BLOCK // 128, band + 2 * EDGE, 128), f32),
            pltpu.VMEM((BLOCK // 128, band + 2 * EDGE, 128), f32),
            pltpu.VMEM((8 * (padded + 8), 128), f32),
            pltpu.VMEM((2 * R * G, 128), f32),
            pltpu.VMEM((1, 128), f32),
            pltpu.SMEM((1, 2, pgy, pgx), jnp.int32),
            dma, dma((3,)), pltpu.SemaphoreType.REGULAR((4,)), dma, dma((arrivals,)), dma, dma,
            dma, dma,
            pltpu.VMEM((G, band + 2 * EDGE, LATE * BLOCK + 2 * SIDE), bf16),
            pltpu.VMEM((1, 128), jnp.int32), pltpu.VMEM((G, 128), jnp.int32),
            dma((3,)), dma((G,)), dma, dma((G,)), dma,
            pltpu.VMEM((5 * G * 8, 128), f32),
        ],
        compiler_params=pltpu.CompilerParams(collective_id=0, has_side_effects=True, vmem_limit_bytes=40 * 2**20),
    )(pltpu.with_memory_space_constraint(peaks, pltpu.HBM), pltpu.with_memory_space_constraint(sections, pltpu.HBM))
    field, offsets, residual = pl.pallas_call(
        functools.partial(spread_out, pgy, pgx),
        name="spread_out",
        out_shape=(
            jax.ShapeDtypeStruct((1, 2, band, width), f32),
            jax.ShapeDtypeStruct((2, pgy * pgx), f32),
            jax.ShapeDtypeStruct((1, band, width), bf16),
        ),
        in_specs=[vmem, vmem],
        out_specs=(anywhere, vmem, anywhere),
        scratch_shapes=[pltpu.VMEM((2, 32 if pgy == 1 else band, width), f32), dma, dma],
        compiler_params=pltpu.CompilerParams(vmem_limit_bytes=20 * 2**20),
    )(nodes, residual)
    return field, offsets.reshape(1, 2, pgy, pgx), residual


def solution(mesh):
    return jax.shard_map(
        functools.partial(per_device, mesh.shape["gz"], mesh.shape["rows"]),
        mesh=mesh,
        in_specs=(P("gz", "rows", None), P("gz", None, None, None)),
        out_specs=(P("gz", None, "rows", None), P("gz", None, None, None), P("gz", "rows", None)),
        check_vma=False,
    )
```
